32 devices in a mesh: pts: 16 (over z, x, core), cen: 2 (over y).
Axes of the slice: x: 2, y: 2, z: 4, core: 2. Of those that a mesh axis runs over, the one named last changes fastest.
Arguments:
- states: bfloat16 [8192, 512], P(('pts', 'cen')), may hold values from -48 to 48
- first_weight: bfloat16 [512, 1024], replicated, may hold values from -0.25 to 0.25
- first_bias: float32 [1024], replicated, may hold values from -4 to 4
- second_weight: bfloat16 [1024, 256], replicated, may hold values from -0.1875 to 0.1875
- centroids: bfloat16 [2, 4096, 256], P('cen'), may hold values from -3.59375 to 3.59375
Outputs:
- new_centroids: float32 [2, 4096, 256], P('cen', 'pts')
- sample_blended_penalty: float32 [8192], P(('pts', 'cen'))
The draws below stay inside these ranges and needn't reach their ends.
All inputs are finite; a program needn't handle non-finite values.
Results may differ from the reference program's by a relative error of at most 0.0061.
Values may be sent and summed in bfloat16 or wider, within the bound.
A program may use at most 128 MiB of HBM per device.

```python
import math
import jax
import jax.numpy as jnp
from jax import lax

SD = 512
HID = 1024
E = 256
K_DEV = 4096
NPTS = 8192
N_CEN = 2


def draw_states(key, part):
    first_key = jax.random.fold_in(jax.random.fold_in(key, 11), 0)
    base = jnp.clip(jax.random.normal(first_key, (NPTS, SD), jnp.float32), -6.0, 6.0)
    return base.astype(jnp.bfloat16)


def levels(key, shape, cuts, smallest, high):
    def one(position, parts):
        heights = jax.random.uniform(jax.random.fold_in(jax.random.fold_in(key, 6), position), (parts,), jnp.float32, smallest / len(cuts), high / len(cuts))
        return jnp.repeat(jnp.exp(heights), shape[position] // parts).reshape((-1,) + (1,) * (len(shape) - position - 1))

    gain = one(*cuts[0])
    for cut in cuts[1:]:
        gain = gain * one(*cut)
    return gain


def bell_draw(own_key, dims, width, limit, pieces=(), held_as=jnp.bfloat16):
    result = width * jax.random.normal(own_key, dims, jnp.float32)
    if pieces:
        result = result * levels(own_key, dims, pieces, -0.22, 0.18)
    return jnp.clip(result, -limit, limit).astype(held_as)


def setup_inputs(seed: int = 0) -> dict:
    arg_keys = jax.random.split(jax.random.key(seed), 6)
    states = draw_states(jax.random.fold_in(arg_keys[5], 71), 0)
    first_weight = bell_draw(arg_keys[1], (SD, HID), SD ** -0.5, 0.25)
    first_bias = bell_draw(arg_keys[2], (HID,), 1.0, 4.0, (), jnp.float32)
    second_weight = bell_draw(arg_keys[3], (HID, E), HID ** -0.5, 0.1875)
    centroids = bell_draw(arg_keys[4], (N_CEN, K_DEV, E), 0.6, 3.59375, ((0, 2),))
    return {"states": states, "first_weight": first_weight, "first_bias": first_bias, "second_weight": second_weight, "centroids": centroids}


smoothing_scale = 16.0


def encode(states, first_weight, first_bias, second_weight):
    pre = jnp.dot(states, first_weight, preferred_element_type=jnp.float32) + first_bias
    hidden = jax.nn.gelu(pre).astype(jnp.bfloat16)
    return jnp.dot(hidden, second_weight, preferred_element_type=jnp.float32).astype(jnp.bfloat16)


def scores_of(rows, centers):
    inner_pairing_matrix = lax.dot_general(rows, centers, (((1,), (1,)), ((), ())), preferred_element_type=jnp.float32)
    sample_length_squared = jnp.sum(jnp.square(rows.astype(jnp.float32)), axis=1)
    center_length_squared = jnp.sum(jnp.square(centers.astype(jnp.float32)), axis=1)
    return (2.0 * inner_pairing_matrix - center_length_squared[None, :] - sample_length_squared[:, None]) / smoothing_scale


def reference(states, first_weight, first_bias, second_weight, centroids):
    codes = encode(states, first_weight, first_bias, second_weight)
    embedding_dimension = codes.shape[1]
    centers = centroids.reshape(-1, embedding_dimension)
    total_rows = codes.shape[0]
    row_block = math.gcd(total_rows, 1024)

    def row_stats(block):
        scores = scores_of(block, centers)
        running_maximum = jnp.max(scores, axis=1)
        running_sum = jnp.sum(jnp.exp(scores - running_maximum[:, None]), axis=1)
        return running_maximum, running_sum

    tracked_peaks, tracked_totals = lax.map(row_stats, codes.reshape(total_rows // row_block, row_block, embedding_dimension))
    tracked_peaks = tracked_peaks.reshape(-1)
    tracked_totals = tracked_totals.reshape(-1)
    sample_blended_penalty = -(smoothing_scale / embedding_dimension) * (tracked_peaks + jnp.log(tracked_totals))
    count_centers = centers.shape[0]
    center_block = math.gcd(count_centers, 1024)

    def center_sums(group):
        scores = scores_of(codes, group)
        resp = jnp.exp(scores - tracked_peaks[:, None]) / tracked_totals[:, None]
        counts = jnp.sum(resp, axis=0)
        weighted = lax.dot_general(resp.astype(jnp.bfloat16), codes, (((0,), (0,)), ((), ())), preferred_element_type=jnp.float32)
        return weighted, counts

    weighted, counts = lax.map(center_sums, centers.reshape(count_centers // center_block, center_block, embedding_dimension))
    weighted = weighted.reshape(count_centers, embedding_dimension)
    counts = counts.reshape(count_centers)
    fresh = (weighted + centers.astype(jnp.float32)) / (counts + 1.0)[:, None]
    return fresh.reshape(centroids.shape), sample_blended_penalty
```

```python
import functools
import math

import jax
import jax.numpy as jnp
from jax import lax
from jax.experimental import pallas as pl
from jax.experimental.pallas import tpu as pltpu
from jax.sharding import PartitionSpec as P

smoothing_scale = 16.0
LOG2E = math.log2(math.e)
MESH = pl.DeviceIdType.MESH
NT = (((1,), (1,)), ((), ()))
PIECES = 4
HALF = PIECES // 2


def kernel(
    n_pts, n_cen, states_hbm, first_hbm, bias_hbm, second_hbm, cen_hbm, out_ref, pen_ref,
    states_ref, first_ref, bias_ref, second_ref, cen_ref, load_sem,
    allc, stat, norm, squares, weighted, counts, other_sums, other_counts,
    line_sem, c_sem, c_rest, x_sem, x_rest, d_sem, stat_sem, norm_sem, pair_sem,
    send_up, send_down, send_x, send_c, send_stat, send_norm, send_pair, token,
):
    n, width = states_ref.shape[0], second_ref.shape[1]
    n_z, others = n_pts // 4, n_cen - 1
    n_own = out_ref.shape[0]
    piece = n // PIECES

    def load(i, src, dst):
        return pltpu.make_async_copy(src, dst, load_sem.at[i])

    load_states = load(0, states_hbm, states_ref)
    load_first = load(1, first_hbm, first_ref)
    load_bias = load(2, bias_hbm, bias_ref)
    load_second = load(3, second_hbm, second_ref)
    load_cen = load(4, cen_hbm.at[0], cen_ref)
    for copy in (load_states, load_first, load_bias, load_second):
        copy.start()

    p, c = lax.axis_index("pts"), lax.axis_index("cen")
    core, x, z = lax.rem(p, 2), lax.rem(p // 2, 2), p // 4
    has_up, has_down = z < n_z - 1, z > 0

    def at(zi, xi, ki):
        return (zi * 2 + xi) * 2 + ki

    def c_at(j):
        return lax.rem(c + j, n_cen)

    def block(zi, xi, ci):
        return (zi * 2 + xi) * n_cen + ci

    up_peer = (at(lax.rem(z + 1, n_z), x, core), c)
    down_peer = (at(lax.rem(z + n_z - 1, n_z), x, core), c)
    x_peer = (at(z, 1 - x, core), c)
    core_peer = (at(z, x, 1 - core), c)
    mine = block(z, x, c)

    barrier = pltpu.get_barrier_semaphore()

    def greet(peer):
        pl.semaphore_signal(barrier, inc=1, device_id=peer, device_id_type=MESH)

    pl.when(has_up)(lambda: greet(up_peer))
    pl.when(has_down)(lambda: greet(down_peer))
    greet(x_peer)
    greet(core_peer)
    for j in range(1, n_cen):
        greet((p, c_at(j)))
    greetings = 2 + others + has_up.astype(jnp.int32) + has_down.astype(jnp.int32)

    def rows_of(q, count=1):
        return pl.ds(q * piece, count * piece)

    def remote(src, dst, send, recv, peer):
        return pltpu.make_async_remote_copy(
            src_ref=src, dst_ref=dst, send_sem=send, recv_sem=recv,
            device_id=peer, device_id_type=MESH,
        )

    def send(b, q, send_sem, recv_sem, peer):
        ref = allc.at[b, rows_of(q)]
        remote(ref, ref, send_sem, recv_sem, peer).start()

    def arrived(ref, recv_sem):
        remote(ref, ref, send_x, recv_sem, core_peer).wait_recv()

    def seat(zi, j):
        return zi * others + j - 1

    def c_slot(zi, j, q):
        return c_sem.at[seat(zi, j), q] if q < HALF else c_rest.at[seat(zi, j)]

    def x_slot(zi, q):
        return x_rest.at[zi] if q < HALF else x_sem.at[zi, q - HALF]

    def at_distance(d, visit):
        if d == 0:
            visit(z)
            return
        pl.when(z + d < n_z)(lambda: visit(z + d))
        pl.when(z >= d)(lambda: visit(z - d))

    def spread(zi, q):
        b = block(zi, x, c)
        pl.when(jnp.logical_and(has_up, zi <= z))(
            lambda: send(b, q, send_up, line_sem.at[zi, q], up_peer)
        )
        pl.when(jnp.logical_and(has_down, zi >= z))(
            lambda: send(b, q, send_down, line_sem.at[zi, q], down_peer)
        )
        for j in range(1, n_cen):
            send(b, q, send_c, c_slot(zi, n_cen - j, q), (p, c_at(j)))
        send(b, q, send_x, x_slot(zi, q), x_peer)

    def line_step(d, q):
        def visit(zi):
            arrived(allc.at[block(zi, x, c), rows_of(q)], line_sem.at[zi, q])
            spread(zi, q)

        at_distance(d, visit)

    def cross_step(d, q):
        def visit(zi):
            if q < HALF:
                for j in range(1, n_cen):
                    b = block(zi, x, c_at(j))
                    arrived(allc.at[b, rows_of(q)], c_slot(zi, j, q))
                    send(b, q, send_x, d_sem.at[seat(zi, j)], x_peer)
            else:
                b = block(zi, 1 - x, c)
                arrived(allc.at[b, rows_of(q)], x_slot(zi, q))
                for j in range(1, n_cen):
                    send(b, q, send_c, d_sem.at[seat(zi, n_cen - j)], (p, c_at(j)))

        at_distance(d, visit)

    with jax.named_scope("load"):
        load_states.wait()
        load_first.wait()
        load_bias.wait()
        load_cen.start()
    part = n // 2
    for h in range(2):
        rows = pl.ds(h * part, part)
        with jax.named_scope(f"encode{h}"):
            pre = jnp.dot(states_ref[rows, :], first_ref[...], preferred_element_type=jnp.float32)
            hidden = jax.nn.gelu(pre + bias_ref[...][None, :]).astype(jnp.bfloat16)
            if h == 0:
                load_second.wait()
            allc[mine, rows, :] = jnp.dot(
                hidden, second_ref[...], preferred_element_type=jnp.float32
            ).astype(jnp.bfloat16)
        if h == 0:
            with jax.named_scope("barrier"):
                pl.semaphore_wait(barrier, greetings)
        for q in range(h * HALF, (h + 1) * HALF):
            spread(z, q)

    def tell(i, peer):
        pl.semaphore_signal(token.at[i], inc=1, device_id=peer, device_id_type=MESH)

    pl.when(z == 0)(lambda: tell(0, up_peer))
    pl.when(z == n_z - 1)(lambda: tell(1, down_peer))

    def pass_on(s):
        @pl.when(jnp.logical_and(has_down, z == s + 1))
        def _():
            pl.semaphore_wait(token.at[0], 1)
            pl.when(has_up)(lambda: tell(0, up_peer))

        @pl.when(jnp.logical_and(has_up, 2 * (n_z - 2 - z) == s))
        def _():
            pl.semaphore_wait(token.at[1], 1)
            pl.when(has_down)(lambda: tell(1, down_peer))

        if s == 2 * (n_z - 2):
            tell(2, x_peer)

    tile = min(512, cen_ref.shape[0])
    tiles = cen_ref.shape[0] // tile
    scale = 2.0 * LOG2E / smoothing_scale

    def tile_rows(i):
        return pl.ds(pl.multiple_of(i * tile, tile), tile)

    def square_step(i, _):
        wide = cen_ref[tile_rows(i), :].astype(jnp.float32)
        total = jnp.sum(wide * wide, axis=1, keepdims=True) * (LOG2E / smoothing_scale)
        squares[tile_rows(i), :] = jnp.broadcast_to(total, (tile, 128))
        return 0

    def less_squares(scores, rows):
        offset = squares[rows, :]
        return jnp.concatenate(
            [scores[:, q * 128:(q + 1) * 128] * scale - offset for q in range(scores.shape[1] // 128)],
            axis=1,
        )

    def stats_step(b, i, carry):
        peak, total = carry
        scores = lax.dot_general(
            cen_ref[tile_rows(i), :], allc[b], NT, preferred_element_type=jnp.float32
        )
        scores = less_squares(scores, tile_rows(i)).reshape(tile // 8, 8, n)
        peak_next = jnp.maximum(peak, jnp.max(scores, axis=0))
        total_next = total * jnp.exp2(peak - peak_next) + jnp.sum(
            jnp.exp2(scores - peak_next[None]), axis=0
        )
        return peak_next, total_next

    group_rows = n * n_cen

    def keep_stats(j, carry):
        peak, total = carry
        top = jnp.max(peak, axis=0, keepdims=True)
        mass = jnp.sum(total * jnp.exp2(peak - top), axis=0, keepdims=True)
        start = pl.multiple_of(c_at(j) * n, n)
        stat[c, :, pl.ds(start, n)] = top
        stat[c, :, pl.ds(group_rows + start, n)] = mass

    fresh = (jnp.full((8, n), -jnp.inf, jnp.float32), jnp.zeros((8, n), jnp.float32))

    with jax.named_scope("squares"):
        load_cen.wait()
        lax.fori_loop(0, tiles, square_step, 0)
    with jax.named_scope("stats_own"):
        keep_stats(0, lax.fori_loop(0, tiles, functools.partial(stats_step, mine), fresh))
    wide = allc[mine].astype(jnp.float32)
    lengths = lax.dot_general(
        jnp.ones((8, width), jnp.float32), wide * wide, NT,
        preferred_element_type=jnp.float32, precision=lax.Precision.HIGHEST,
    )
    weighted[...] = jnp.zeros_like(weighted)
    counts[...] = jnp.zeros_like(counts)

    pair = pl.ds(pl.multiple_of((p - core) * n_own, 2 * n_own), 2 * n_own)

    def consume(b, g, ci):
        rows = allc[b]
        scores = lax.dot_general(cen_ref[pair, :], rows, NT, preferred_element_type=jnp.float32)
        level = norm[g, :, pl.ds(pl.multiple_of(ci * n, n), n)]
        resp = jnp.exp2(less_squares(scores, pair) - level)
        lanes = resp[:, 0:128]
        for q in range(1, n // 128):
            lanes = lanes + resp[:, q * 128:(q + 1) * 128]
        counts[...] += lanes.reshape(counts.shape)
        weighted[...] += jnp.dot(
            resp.astype(jnp.bfloat16), rows, preferred_element_type=jnp.float32
        ).reshape(weighted.shape)

    def ordered(i):
        near = jnp.minimum(z, n_z - 1 - z)
        beside = z + (i + 1) // 2 if i % 2 else z - i // 2
        beyond = jnp.where(z <= n_z - 1 - z, i, n_z - 1 - i)
        return jnp.where(i <= 2 * near, beside, beyond)

    def rest_of(b, q, sem):
        arrived(allc.at[b, rows_of(q, HALF)], sem)

    def norm_arrived(zi, xi):
        g = zi * 2 + xi
        arrived(norm.at[g], norm_sem.at[g])

    def take_line(i):
        zi = ordered(i)
        if i > 0:
            norm_arrived(zi, x)
        consume(block(zi, x, c), zi * 2 + x, c)

    def take_c(i):
        zi = ordered(i)

        def one(j, _):
            b = block(zi, x, c_at(j))
            if i > 0:
                rest_of(b, HALF, c_rest.at[seat(zi, j)])
            consume(b, zi * 2 + x, c_at(j))
            return 0

        lax.fori_loop(1, n_cen, one, 0, unroll=others == 1)

    def take_x(i):
        zi = ordered(i)
        norm_arrived(zi, 1 - x)
        rest_of(block(zi, 1 - x, c), 0, x_rest.at[zi])
        consume(block(zi, 1 - x, c), zi * 2 + 1 - x, c)

    def take_d(i):
        zi = ordered(i)

        def one(j, _):
            b = block(zi, 1 - x, c_at(j))
            arrived(allc.at[b], d_sem.at[seat(zi, j)])
            consume(b, zi * 2 + 1 - x, c_at(j))
            return 0

        lax.fori_loop(1, n_cen, one, 0, unroll=others == 1)

    def stats_cross(first, last, carry):
        nxt = []
        for j in range(1, n_cen):
            step = functools.partial(stats_step, block(z, x, c_at(j)))
            nxt.append(lax.fori_loop(first, last, step, carry[j - 1]))
        return nxt

    def share_stats():
        for j in range(1, n_cen):
            remote(
                stat.at[c], stat.at[c], send_stat, stat_sem.at[n_cen - j - 1], (p, c_at(j))
            ).start()

    def share_norm():
        for j in range(1, n_cen):
            s = c_at(j)
            arrived(stat.at[s], stat_sem.at[j - 1])
        top = stat[0, :, 0:group_rows]
        for s in range(1, n_cen):
            top = jnp.maximum(top, stat[s, :, 0:group_rows])
        mass = jnp.zeros_like(top)
        for s in range(n_cen):
            mass = mass + stat[s, :, group_rows:2 * group_rows] * jnp.exp2(
                stat[s, :, 0:group_rows] - top
            )
        level = top + jnp.log(mass) * LOG2E
        g = z * 2 + x
        norm[g] = level
        pl.semaphore_wait(token.at[2], 1)
        for k in range(1, 2 * n_z):
            h = lax.rem(g + k, 2 * n_z)
            remote(norm.at[g], norm.at[g], send_norm, norm_sem.at[g], (h * 2 + core, c)).start()
        own = norm[g, :, pl.ds(pl.multiple_of(c * n, n), n)]
        pen_ref[...] = (-(smoothing_scale / width)) * (
            own * math.log(2.0) - lengths[0:1, :] / smoothing_scale
        )

    tasks = []
    for i in range(n_z):
        tasks += [
            functools.partial(take_line, i), functools.partial(take_c, i),
            functools.partial(take_x, i), functools.partial(take_d, i),
        ]
    if n_z > 1:
        swap = tasks[-6:]
        tasks[-6:] = [swap[0], swap[2], swap[1], swap[3], swap[4], swap[5]]
    total_steps = n_z * PIECES
    first_take = 2 * PIECES + 2
    carry = [fresh] * others
    done = 0
    for s in range(total_steps):
        d, q = 1 + s // PIECES, s % PIECES
        with jax.named_scope(f"move{s}"):
            if d < n_z:
                line_step(d, q)
            cross_step(d - 1, q)
            if s <= max(n_z - 2, 2 * (n_z - 2)):
                pass_on(s)
        with jax.named_scope(f"work{s}"):
            if s == PIECES - 1:
                for j in range(1, n_cen):
                    rest_of(block(z, x, c_at(j)), HALF, c_rest.at[seat(z, j)])
            if PIECES <= s < 2 * PIECES:
                k = s - PIECES
                carry = stats_cross(tiles * k // PIECES, tiles * (k + 1) // PIECES, carry)
            if s == 2 * PIECES - 1:
                for j in range(1, n_cen):
                    keep_stats(j, carry[j - 1])
                share_stats()
            if s == 2 * PIECES + 1:
                share_norm()
            if s >= first_take:
                until = len(tasks) * (s - first_take + 1) // (total_steps - first_take + 2)
                for task in tasks[done:until]:
                    task()
                done = until
    with jax.named_scope("tail"):
        for task in tasks[done:]:
            task()

    with jax.named_scope("pair"):
        sums = remote(
            weighted.at[1 - core], other_sums, send_pair.at[0], pair_sem.at[0], core_peer
        )
        tally = remote(
            counts.at[1 - core], other_counts, send_pair.at[1], pair_sem.at[1], core_peer
        )
        tally.start()
        sums.start()
        own_rows = pl.ds(pl.multiple_of(p * n_own, n_own), n_own)
        tally.wait()
        share = 1.0 / (
            jnp.sum(counts[core] + other_counts[...], axis=1, keepdims=True) + 1.0
        )
        sums.wait()
    with jax.named_scope("final"):
        out_ref[...] = (
            weighted[core] + other_sums[...] + cen_ref[own_rows, :].astype(jnp.float32)
        ) * share

    with jax.named_scope("sent"):

        def left(ref, send_sem):
            remote(ref, ref, send_sem, pair_sem.at[0], core_peer).wait_send()

        across = n_z + n_z * others // 2
        left(allc.at[pl.ds(0, across)], send_x)
        left(allc.at[pl.ds(0, others * (n_z + n_z // 2))], send_c)
        for zi in range(n_z - 1):
            pl.when(z == zi)(lambda zi=zi: left(allc.at[pl.ds(0, zi + 1)], send_up))
            pl.when(z == n_z - 1 - zi)(lambda zi=zi: left(allc.at[pl.ds(0, zi + 1)], send_down))
        left(stat.at[pl.ds(0, others)], send_stat)
        left(norm.at[pl.ds(0, 2 * n_z - 1)], send_norm)


def finish(fresh_ref, pen_ref, out_ref, cost_ref):
    out_ref[0] = fresh_ref[...]
    cost_ref[...] = pen_ref[0]


def body(n_pts, n_cen, states, first_weight, first_bias, second_weight, centroids):
    n, width = states.shape[0], second_weight.shape[1]
    k_dev = centroids.shape[1]
    owned = k_dev // n_pts
    n_z, others = n_pts // 4, n_cen - 1
    dma = pltpu.SemaphoreType.DMA
    vmem, f32 = pltpu.VMEM, jnp.float32
    args = [
        pltpu.with_memory_space_constraint(v, pltpu.HBM)
        for v in (states, first_weight, first_bias, second_weight, centroids)
    ]
    fresh, penalty = pl.pallas_call(
        functools.partial(kernel, n_pts, n_cen),
        out_shape=(vmem((owned, width), f32), vmem((1, n), f32)),
        in_specs=[pl.BlockSpec(memory_space=pltpu.HBM)] * 5,
        out_specs=(pl.BlockSpec(memory_space=vmem),) * 2,
        scratch_shapes=[
            vmem(states.shape, states.dtype),
            vmem(first_weight.shape, first_weight.dtype),
            vmem(first_bias.shape, first_bias.dtype),
            vmem(second_weight.shape, second_weight.dtype),
            vmem(centroids.shape[1:], centroids.dtype),
            dma((5,)),
            vmem((2 * n_z * n_cen, n, width), jnp.bfloat16),
            vmem((n_cen, 1, 2 * n_cen * n), f32),
            vmem((2 * n_z, 1, n_cen * n), f32),
            vmem((k_dev, 128), f32),
            vmem((2, owned, width), f32),
            vmem((2, owned, 128), f32),
            vmem((owned, width), f32),
            vmem((owned, 128), f32),
            dma((n_z, PIECES)),
            dma((n_z * others, HALF)),
            dma((n_z * others,)),
            dma((n_z, HALF)),
            dma((n_z,)),
            dma((n_z * others,)),
            dma((others,)),
            dma((2 * n_z,)),
            dma((2,)),
            dma, dma, dma, dma, dma, dma,
            dma((2,)),
            pltpu.SemaphoreType.REGULAR((3,)),
        ],
        compiler_params=pltpu.CompilerParams(
            collective_id=0, has_side_effects=True, vmem_limit_bytes=48 * 1024 * 1024
        ),
    )(*args)
    return pl.pallas_call(
        finish,
        out_shape=(
            jax.ShapeDtypeStruct((1, owned, width), f32),
            jax.ShapeDtypeStruct((n,), f32),
        ),
        in_specs=[pl.BlockSpec(memory_space=vmem)] * 2,
        out_specs=(pl.BlockSpec(memory_space=vmem),) * 2,
        compiler_params=pltpu.CompilerParams(vmem_limit_bytes=4 * 1024 * 1024),
    )(fresh, penalty)


def solution(mesh):
    placed = (P(("pts", "cen"), None), P(), P(), P(), P("cen", None, None))
    return jax.shard_map(
        functools.partial(body, mesh.shape["pts"], mesh.shape["cen"]),
        mesh=mesh,
        in_specs=placed,
        out_specs=(P("cen", "pts", None), P(("pts", "cen"))),
        check_vma=False,
    )
```

```python
import functools
import math

import jax
import jax.numpy as jnp
from jax import lax
from jax.experimental import pallas as pl
from jax.experimental.pallas import tpu as pltpu
from jax.sharding import PartitionSpec as P

smoothing_scale = 16.0
LOG2E = math.log2(math.e)
MESH = pl.DeviceIdType.MESH
NT = (((1,), (1,)), ((), ()))
PIECES = 4
HALF = PIECES // 2


def kernel(
    n_pts, n_cen, states_hbm, first_hbm, bias_hbm, second_hbm, cen_hbm, out_ref, pen_ref,
    states_ref, first_ref, bias_ref, second_ref, cen_ref, load_sem,
    allc, stat, norm, squares, weighted, counts, other_sums, other_counts,
    line_sem, c_sem, c_rest, x_sem, x_rest, d_sem, stat_sem, norm_sem, pair_sem,
    send_up, send_down, send_x, send_c, send_stat, send_norm, send_pair, token,
):
    n, width = states_ref.shape[0], second_ref.shape[1]
    n_z, others = n_pts // 4, n_cen - 1
    n_own = out_ref.shape[0]
    piece = n // PIECES

    def load(i, src, dst):
        return pltpu.make_async_copy(src, dst, load_sem.at[i])

    load_states = load(0, states_hbm, states_ref)
    load_first = load(1, first_hbm, first_ref)
    load_bias = load(2, bias_hbm, bias_ref)
    load_second = load(3, second_hbm, second_ref)
    load_cen = load(4, cen_hbm.at[0], cen_ref)
    for copy in (load_states, load_first, load_bias, load_second):
        copy.start()

    p, c = lax.axis_index("pts"), lax.axis_index("cen")
    core, x, z = lax.rem(p, 2), lax.rem(p // 2, 2), p // 4
    has_up, has_down = z < n_z - 1, z > 0

    def at(zi, xi, ki):
        return (zi * 2 + xi) * 2 + ki

    def c_at(j):
        return lax.rem(c + j, n_cen)

    def block(zi, xi, ci):
        return (zi * 2 + xi) * n_cen + ci

    up_peer = (at(lax.rem(z + 1, n_z), x, core), c)
    down_peer = (at(lax.rem(z + n_z - 1, n_z), x, core), c)
    x_peer = (at(z, 1 - x, core), c)
    core_peer = (at(z, x, 1 - core), c)
    mine = block(z, x, c)

    barrier = pltpu.get_barrier_semaphore()

    def greet(peer):
        pl.semaphore_signal(barrier, inc=1, device_id=peer, device_id_type=MESH)

    pl.when(has_up)(lambda: greet(up_peer))
    pl.when(has_down)(lambda: greet(down_peer))
    greet(x_peer)
    greet(core_peer)
    for j in range(1, n_cen):
        greet((p, c_at(j)))
    greetings = 2 + others + has_up.astype(jnp.int32) + has_down.astype(jnp.int32)

    def rows_of(q, count=1):
        return pl.ds(q * piece, count * piece)

    def remote(src, dst, send, recv, peer):
        return pltpu.make_async_remote_copy(
            src_ref=src, dst_ref=dst, send_sem=send, recv_sem=recv,
            device_id=peer, device_id_type=MESH,
        )

    def send(b, q, send_sem, recv_sem, peer):
        ref = allc.at[b, rows_of(q)]
        remote(ref, ref, send_sem, recv_sem, peer).start()

    def arrived(ref, recv_sem):
        remote(ref, ref, send_x, recv_sem, core_peer).wait_recv()

    def seat(zi, j):
        return zi * others + j - 1

    def c_slot(zi, j, q):
        return c_sem.at[seat(zi, j), q] if q < HALF else c_rest.at[seat(zi, j)]

    def x_slot(zi, q):
        return x_rest.at[zi] if q < HALF else x_sem.at[zi, q - HALF]

    def at_distance(d, visit):
        if d == 0:
            visit(z)
            return
        pl.when(z + d < n_z)(lambda: visit(z + d))
        pl.when(z >= d)(lambda: visit(z - d))

    def along(zi, q):
        b = block(zi, x, c)
        pl.when(jnp.logical_and(has_up, zi <= z))(
            lambda: send(b, q, send_up, line_sem.at[zi, q], up_peer)
        )
        pl.when(jnp.logical_and(has_down, zi >= z))(
            lambda: send(b, q, send_down, line_sem.at[zi, q], down_peer)
        )

    def aside(zi, q):
        b = block(zi, x, c)
        for j in range(1, n_cen):
            send(b, q, send_c, c_slot(zi, n_cen - j, q), (p, c_at(j)))
        send(b, q, send_x, x_slot(zi, q), x_peer)

    def line_step(d, q):
        def visit(zi):
            arrived(allc.at[block(zi, x, c), rows_of(q)], line_sem.at[zi, q])
            along(zi, q)

        at_distance(d, visit)

    def ordered(i):
        near = jnp.minimum(z, n_z - 1 - z)
        beside = z + (i + 1) // 2 if i % 2 else z - i // 2
        beyond = jnp.where(z <= n_z - 1 - z, i, n_z - 1 - i)
        return jnp.where(i <= 2 * near, beside, beyond)

    def cross_step(i, q):
        zi = ordered(i)
        if q < HALF:
            for j in range(1, n_cen):
                b = block(zi, x, c_at(j))
                arrived(allc.at[b, rows_of(q)], c_slot(zi, j, q))
                send(b, q, send_x, d_sem.at[seat(zi, j)], x_peer)
        else:
            b = block(zi, 1 - x, c)
            arrived(allc.at[b, rows_of(q)], x_slot(zi, q))
            for j in range(1, n_cen):
                send(b, q, send_c, d_sem.at[seat(zi, n_cen - j)], (p, c_at(j)))

    with jax.named_scope("load"):
        load_states.wait()
        load_first.wait()
        load_bias.wait()
        load_cen.start()
    part = n // 2
    for h in range(2):
        rows = pl.ds(h * part, part)
        with jax.named_scope(f"encode{h}"):
            pre = jnp.dot(states_ref[rows, :], first_ref[...], preferred_element_type=jnp.float32)
            hidden = jax.nn.gelu(pre + bias_ref[...][None, :]).astype(jnp.bfloat16)
            if h == 0:
                load_second.wait()
            allc[mine, rows, :] = jnp.dot(
                hidden, second_ref[...], preferred_element_type=jnp.float32
            ).astype(jnp.bfloat16)
        if h == 0:
            with jax.named_scope("barrier"):
                pl.semaphore_wait(barrier, greetings)
        for q in range(h * HALF, (h + 1) * HALF):
            along(z, q)
            aside(z, q)

    def tell(i, peer):
        pl.semaphore_signal(token.at[i], inc=1, device_id=peer, device_id_type=MESH)

    pl.when(z == 0)(lambda: tell(0, up_peer))
    pl.when(z == n_z - 1)(lambda: tell(1, down_peer))

    def pass_on(s):
        @pl.when(jnp.logical_and(has_down, z == s + 1))
        def _():
            pl.semaphore_wait(token.at[0], 1)
            pl.when(has_up)(lambda: tell(0, up_peer))

        @pl.when(jnp.logical_and(has_up, 2 * (n_z - 2 - z) == s))
        def _():
            pl.semaphore_wait(token.at[1], 1)
            pl.when(has_down)(lambda: tell(1, down_peer))

        if s == 2 * (n_z - 2):
            tell(2, x_peer)

    tile = min(512, cen_ref.shape[0])
    tiles = cen_ref.shape[0] // tile
    scale = 2.0 * LOG2E / smoothing_scale

    def tile_rows(i):
        return pl.ds(i * tile, tile) if isinstance(i, int) else pl.ds(pl.multiple_of(i * tile, tile), tile)

    def square_step(i):
        wide = cen_ref[tile_rows(i), :].astype(jnp.float32)
        total = jnp.sum(wide * wide, axis=1, keepdims=True) * (LOG2E / smoothing_scale)
        squares[tile_rows(i), :] = jnp.broadcast_to(total, (tile, 128))

    def less_squares(scores, rows):
        offset = squares[rows, :]
        return jnp.concatenate(
            [scores[:, q * 128:(q + 1) * 128] * scale - offset for q in range(scores.shape[1] // 128)],
            axis=1,
        )

    def stats_step(b, i, carry):
        peak, total = carry
        scores = lax.dot_general(
            cen_ref[tile_rows(i), :], allc[b], NT, preferred_element_type=jnp.float32
        )
        scores = less_squares(scores, tile_rows(i)).reshape(tile // 8, 8, n)
        peak_next = jnp.maximum(peak, jnp.max(scores, axis=0))
        total_next = total * jnp.exp2(peak - peak_next) + jnp.sum(
            jnp.exp2(scores - peak_next[None]), axis=0
        )
        return peak_next, total_next

    group_rows = n * n_cen

    def keep_stats(j, carry):
        peak, total = carry
        top = jnp.max(peak, axis=0, keepdims=True)
        mass = jnp.sum(total * jnp.exp2(peak - top), axis=0, keepdims=True)
        start = pl.multiple_of(c_at(j) * n, n)
        stat[c, :, pl.ds(start, n)] = top
        stat[c, :, pl.ds(group_rows + start, n)] = mass

    fresh = (jnp.full((8, n), -jnp.inf, jnp.float32), jnp.zeros((8, n), jnp.float32))

    with jax.named_scope("cen"):
        load_cen.wait()
    with jax.named_scope("stats_own"):
        running = fresh
        for i in range(tiles):
            square_step(i)
            running = stats_step(mine, i, running)
        keep_stats(0, running)
    wide = allc[mine].astype(jnp.float32)
    lengths = lax.dot_general(
        jnp.ones((8, width), jnp.float32), wide * wide, NT,
        preferred_element_type=jnp.float32, precision=lax.Precision.HIGHEST,
    )
    weighted[...] = jnp.zeros_like(weighted)
    counts[...] = jnp.zeros_like(counts)

    pair = pl.ds(pl.multiple_of((p - core) * n_own, 2 * n_own), 2 * n_own)

    def consume(b, g, ci, count=1):
        span = count * n
        rows = allc[pl.ds(b, count)].reshape(span, width)
        scores = lax.dot_general(cen_ref[pair, :], rows, NT, preferred_element_type=jnp.float32)
        level = norm[g, :, pl.ds(pl.multiple_of(ci * n, n), span)]
        resp = jnp.exp2(less_squares(scores, pair) - level)
        lanes = resp[:, 0:128]
        for q in range(1, span // 128):
            lanes = lanes + resp[:, q * 128:(q + 1) * 128]
        counts[...] += lanes.reshape(counts.shape)
        weighted[...] += jnp.dot(
            resp.astype(jnp.bfloat16), rows, preferred_element_type=jnp.float32
        ).reshape(weighted.shape)

    def consume_group(g):
        if n_cen <= 2:
            consume(g * n_cen, g, 0, n_cen)
            return

        def one(ci, _):
            consume(g * n_cen + ci, g, ci)
            return 0

        lax.fori_loop(0, n_cen, one, 0)

    def rest_of(b, q, sem):
        arrived(allc.at[b, rows_of(q, HALF)], sem)

    def norm_arrived(zi, xi):
        g = zi * 2 + xi
        arrived(norm.at[g], norm_sem.at[g])

    def take_line(i):
        zi = ordered(i)
        if i > 0:
            norm_arrived(zi, x)
            for j in range(1, n_cen):
                rest_of(block(zi, x, c_at(j)), HALF, c_rest.at[seat(zi, j)])
        consume_group(zi * 2 + x)

    def x_ready(i):
        zi = ordered(i)
        norm_arrived(zi, 1 - x)
        rest_of(block(zi, 1 - x, c), 0, x_rest.at[zi])

    def take_x(i):
        zi = ordered(i)
        x_ready(i)
        for j in range(1, n_cen):
            arrived(allc.at[block(zi, 1 - x, c_at(j))], d_sem.at[seat(zi, j)])
        consume_group(zi * 2 + 1 - x)

    def take_last_b(i):
        zi = ordered(i)
        x_ready(i)
        consume(block(zi, 1 - x, c), zi * 2 + 1 - x, c)

    def take_last_d(i):
        zi = ordered(i)

        def one(j, _):
            b = block(zi, 1 - x, c_at(j))
            arrived(allc.at[b], d_sem.at[seat(zi, j)])
            consume(b, zi * 2 + 1 - x, c_at(j))
            return 0

        lax.fori_loop(1, n_cen, one, 0, unroll=others == 1)

    def stats_cross(first, last, carry):
        nxt = []
        for j in range(1, n_cen):
            step = functools.partial(stats_step, block(z, x, c_at(j)))
            running = carry[j - 1]
            if n_cen <= 2:
                for i in range(first, last):
                    running = step(i, running)
            else:
                running = lax.fori_loop(first, last, step, running)
            nxt.append(running)
        return nxt

    def share_stats():
        for j in range(1, n_cen):
            remote(
                stat.at[c], stat.at[c], send_stat, stat_sem.at[n_cen - j - 1], (p, c_at(j))
            ).start()

    def share_norm():
        for j in range(1, n_cen):
            s = c_at(j)
            arrived(stat.at[s], stat_sem.at[j - 1])
        top = stat[0, :, 0:group_rows]
        for s in range(1, n_cen):
            top = jnp.maximum(top, stat[s, :, 0:group_rows])
        mass = jnp.zeros_like(top)
        for s in range(n_cen):
            mass = mass + stat[s, :, group_rows:2 * group_rows] * jnp.exp2(
                stat[s, :, 0:group_rows] - top
            )
        level = top + jnp.log(mass) * LOG2E
        g = z * 2 + x
        norm[g] = level
        pl.semaphore_wait(token.at[2], 1)
        for k in range(1, 2 * n_z):
            h = lax.rem(g + k, 2 * n_z)
            remote(norm.at[g], norm.at[g], send_norm, norm_sem.at[g], (h * 2 + core, c)).start()
        own = norm[g, :, pl.ds(pl.multiple_of(c * n, n), n)]
        pen_ref[...] = (-(smoothing_scale / width)) * (
            own * math.log(2.0) - lengths[0:1, :] / smoothing_scale
        )

    total_steps = n_z * PIECES
    cross_from, norm_at = PIECES, 2 * PIECES
    takes = [functools.partial(take_line, 0)]
    for i in range(n_z):
        if i > 0:
            takes.append(functools.partial(take_line, i))
        if i < n_z - 1:
            takes.append(functools.partial(take_x, i))
    takes += [functools.partial(take_last_b, n_z - 1), functools.partial(take_last_d, n_z - 1)]
    first_take = norm_at + 1
    held = 3
    carry = [fresh] * others
    done = 0
    for s in range(total_steps):
        i, q = 1 + s // PIECES, s % PIECES
        with jax.named_scope(f"move{s}"):
            if i < n_z:
                line_step(i, q)
                aside(ordered(i), q)
            cross_step(i - 1, q)
            if s <= max(n_z - 2, 2 * (n_z - 2)):
                pass_on(s)
        with jax.named_scope(f"work{s}"):
            if s == PIECES - 1:
                for j in range(1, n_cen):
                    rest_of(block(z, x, c_at(j)), HALF, c_rest.at[seat(z, j)])
            if cross_from <= s < cross_from + 2:
                k = s - cross_from
                carry = stats_cross(tiles * k // 2, tiles * (k + 1) // 2, carry)
                if k == 1:
                    for j in range(1, n_cen):
                        keep_stats(j, carry[j - 1])
                    share_stats()
            if s == norm_at:
                share_norm()
            if s >= first_take:
                until = (len(takes) - held) * (s - first_take + 1) // (total_steps - first_take)
                for take in takes[done:until]:
                    take()
                done = until
    with jax.named_scope("tail"):
        for take in takes[done:]:
            take()

    with jax.named_scope("pair"):
        sums = remote(
            weighted.at[1 - core], other_sums, send_pair.at[0], pair_sem.at[0], core_peer
        )
        tally = remote(
            counts.at[1 - core], other_counts, send_pair.at[1], pair_sem.at[1], core_peer
        )
        tally.start()
        sums.start()
        own_rows = pl.ds(pl.multiple_of(p * n_own, n_own), n_own)
        tally.wait()
        share = 1.0 / (
            jnp.sum(counts[core] + other_counts[...], axis=1, keepdims=True) + 1.0
        )
        sums.wait()
    with jax.named_scope("final"):
        out_ref[...] = (
            weighted[core] + other_sums[...] + cen_ref[own_rows, :].astype(jnp.float32)
        ) * share

    with jax.named_scope("sent"):

        def left(ref, send_sem):
            remote(ref, ref, send_sem, pair_sem.at[0], core_peer).wait_send()

        across = n_z + n_z * others // 2
        left(allc.at[pl.ds(0, across)], send_x)
        left(allc.at[pl.ds(0, others * (n_z + n_z // 2))], send_c)
        for zi in range(n_z - 1):
            pl.when(z == zi)(lambda zi=zi: left(allc.at[pl.ds(0, zi + 1)], send_up))
            pl.when(z == n_z - 1 - zi)(lambda zi=zi: left(allc.at[pl.ds(0, zi + 1)], send_down))
        left(stat.at[pl.ds(0, others)], send_stat)
        left(norm.at[pl.ds(0, 2 * n_z - 1)], send_norm)


def finish(fresh_ref, pen_ref, out_ref, cost_ref):
    out_ref[0] = fresh_ref[...]
    cost_ref[...] = pen_ref[0]


def body(n_pts, n_cen, states, first_weight, first_bias, second_weight, centroids):
    n, width = states.shape[0], second_weight.shape[1]
    k_dev = centroids.shape[1]
    owned = k_dev // n_pts
    n_z, others = n_pts // 4, n_cen - 1
    dma = pltpu.SemaphoreType.DMA
    vmem, f32 = pltpu.VMEM, jnp.float32
    args = [
        pltpu.with_memory_space_constraint(v, pltpu.HBM)
        for v in (states, first_weight, first_bias, second_weight, centroids)
    ]
    fresh, penalty = pl.pallas_call(
        functools.partial(kernel, n_pts, n_cen),
        out_shape=(vmem((owned, width), f32), vmem((1, n), f32)),
        in_specs=[pl.BlockSpec(memory_space=pltpu.HBM)] * 5,
        out_specs=(pl.BlockSpec(memory_space=vmem),) * 2,
        scratch_shapes=[
            vmem(states.shape, states.dtype),
            vmem(first_weight.shape, first_weight.dtype),
            vmem(first_bias.shape, first_bias.dtype),
            vmem(second_weight.shape, second_weight.dtype),
            vmem(centroids.shape[1:], centroids.dtype),
            dma((5,)),
            vmem((2 * n_z * n_cen, n, width), jnp.bfloat16),
            vmem((n_cen, 1, 2 * n_cen * n), f32),
            vmem((2 * n_z, 1, n_cen * n), f32),
            vmem((k_dev, 128), f32),
            vmem((2, owned, width), f32),
            vmem((2, owned, 128), f32),
            vmem((owned, width), f32),
            vmem((owned, 128), f32),
            dma((n_z, PIECES)),
            dma((n_z * others, HALF)),
            dma((n_z * others,)),
            dma((n_z, HALF)),
            dma((n_z,)),
            dma((n_z * others,)),
            dma((others,)),
            dma((2 * n_z,)),
            dma((2,)),
            dma, dma, dma, dma, dma, dma,
            dma((2,)),
            pltpu.SemaphoreType.REGULAR((3,)),
        ],
        compiler_params=pltpu.CompilerParams(
            collective_id=0, has_side_effects=True, vmem_limit_bytes=48 * 1024 * 1024
        ),
    )(*args)
    return pl.pallas_call(
        finish,
        out_shape=(
            jax.ShapeDtypeStruct((1, owned, width), f32),
            jax.ShapeDtypeStruct((n,), f32),
        ),
        in_specs=[pl.BlockSpec(memory_space=vmem)] * 2,
        out_specs=(pl.BlockSpec(memory_space=vmem),) * 2,
        compiler_params=pltpu.CompilerParams(vmem_limit_bytes=4 * 1024 * 1024),
    )(fresh, penalty)


def solution(mesh):
    placed = (P(("pts", "cen"), None), P(), P(), P(), P("cen", None, None))
    return jax.shard_map(
        functools.partial(body, mesh.shape["pts"], mesh.shape["cen"]),
        mesh=mesh,
        in_specs=placed,
        out_specs=(P("cen", "pts", None), P(("pts", "cen"))),
        check_vma=False,
    )
```

```python
import functools
import math

import jax
import jax.numpy as jnp
from jax import lax
from jax.experimental import pallas as pl
from jax.experimental.pallas import tpu as pltpu
from jax.sharding import PartitionSpec as P

smoothing_scale = 16.0
LOG2E = math.log2(math.e)
MESH = pl.DeviceIdType.MESH
NT = (((1,), (1,)), ((), ()))
PIECES = 4
HALF = PIECES // 2


def kernel(
    n_pts, n_cen, states_hbm, first_hbm, bias_hbm, second_hbm, cen_hbm, out_ref, pen_ref,
    states_ref, first_ref, bias_ref, second_ref, cen_ref, load_sem,
    allc, stat, norm, squares, weighted, counts, other_sums, other_counts,
    line_sem, c_sem, c_rest, x_sem, x_rest, d_sem, stat_sem, norm_sem, pair_sem,
    send_up, send_down, send_x, send_c, send_dup, send_ddown, send_dx, send_dc,
    send_stat, send_norm, send_pair, token,
):
    n, width = states_ref.shape[0], second_ref.shape[1]
    n_z, others = n_pts // 4, n_cen - 1
    n_own = out_ref.shape[0]
    piece = n // PIECES

    def load(i, src, dst):
        return pltpu.make_async_copy(src, dst, load_sem.at[i])

    load_states = load(0, states_hbm, states_ref)
    load_first = load(1, first_hbm, first_ref)
    load_bias = load(2, bias_hbm, bias_ref)
    load_second = load(3, second_hbm, second_ref)
    load_cen = load(4, cen_hbm.at[0], cen_ref)
    for copy in (load_states, load_first, load_bias, load_second):
        copy.start()

    p, c = lax.axis_index("pts"), lax.axis_index("cen")
    core, x, z = lax.rem(p, 2), lax.rem(p // 2, 2), p // 4
    has_up, has_down = z < n_z - 1, z > 0

    side = lax.rem(core + x + z + c, 2)

    def at(zi, xi, ci):
        return ((zi * 2 + xi) * 2 + lax.rem(side + xi + zi + ci, 2), ci)

    def c_at(j):
        return lax.rem(c + j, n_cen)

    def block(zi, xi, ci):
        return (zi * 2 + xi) * n_cen + ci

    def c_peer(j):
        return at(z, x, c_at(j))

    up_peer, down_peer = at(lax.rem(z + 1, n_z), x, c), at(lax.rem(z + n_z - 1, n_z), x, c)
    x_peer, core_peer = at(z, 1 - x, c), (p + 1 - 2 * core, c)
    mine = block(z, x, c)

    barrier = pltpu.get_barrier_semaphore()

    def greet(peer):
        pl.semaphore_signal(barrier, inc=1, device_id=peer, device_id_type=MESH)

    pl.when(has_up)(lambda: greet(up_peer))
    pl.when(has_down)(lambda: greet(down_peer))
    greet(x_peer)
    greet(core_peer)
    for j in range(1, n_cen):
        greet(c_peer(j))
    greetings = 2 + others + has_up.astype(jnp.int32) + has_down.astype(jnp.int32)

    def rows_of(q, count=1):
        return pl.ds(q * piece, count * piece)

    def remote(src, dst, send, recv, peer):
        return pltpu.make_async_remote_copy(
            src_ref=src, dst_ref=dst, send_sem=send, recv_sem=recv,
            device_id=peer, device_id_type=MESH,
        )

    def send(b, q, send_sem, recv_sem, peer):
        ref = allc.at[b, rows_of(q)]
        remote(ref, ref, send_sem, recv_sem, peer).start()

    def arrived(ref, recv_sem):
        remote(ref, ref, send_x, recv_sem, core_peer).wait_recv()

    def seat(zi, j):
        return zi * others + j - 1

    def c_slot(zi, j, q):
        return c_sem.at[seat(zi, j), q] if q < HALF else c_rest.at[seat(zi, j)]

    def x_slot(zi, q):
        return x_rest.at[zi] if q < HALF else x_sem.at[zi, q - HALF]

    def at_distance(d, visit):
        if d == 0:
            visit(z)
            return
        pl.when(z + d < n_z)(lambda: visit(z + d))
        pl.when(z >= d)(lambda: visit(z - d))

    def along(zi, q):
        b = block(zi, x, c)
        pl.when(passes_up(zi))(lambda: send(b, q, send_up, line_sem.at[zi, q], up_peer))
        pl.when(passes_down(zi))(lambda: send(b, q, send_down, line_sem.at[zi, q], down_peer))

    def aside(zi, q):
        b = block(zi, x, c)
        for j in range(1, n_cen):
            send(b, q, send_c, c_slot(zi, n_cen - j, q), c_peer(j))
        send(b, q, send_x, x_slot(zi, q), x_peer)

    def passes_up(zi):
        return jnp.logical_and(has_up, zi <= z)

    def passes_down(zi):
        return jnp.logical_and(has_down, zi >= z)

    def passes(zi):
        return jnp.logical_or(passes_up(zi), passes_down(zi))

    def line_arrived(zi, q):
        arrived(allc.at[block(zi, x, c), rows_of(q)], line_sem.at[zi, q])

    def line_forward(d, q):
        def visit(zi):
            @pl.when(passes(zi))
            def _():
                line_arrived(zi, q)
                along(zi, q)

        at_distance(d, visit)

    def line_step(i, q):
        zi = ordered(i)
        pl.when(jnp.logical_not(passes(zi)))(lambda: line_arrived(zi, q))

    def ordered(i):
        near = jnp.minimum(z, n_z - 1 - z)
        beside = z + (i + 1) // 2 if i % 2 else z - i // 2
        beyond = jnp.where(z <= n_z - 1 - z, i, n_z - 1 - i)
        return jnp.where(i <= 2 * near, beside, beyond)

    def d_slot(zi, j, q):
        return d_sem.at[seat(zi, j), q]

    def by_line(q):
        return HALF - 1 <= q <= HALF

    def cross_step(i, q):
        zi = ordered(i)

        def forward(visit):
            if i == 0:
                visit()
            elif not by_line(q):
                pl.when(jnp.abs(zi - z) > 1)(visit)

        for j in range(1, n_cen):
            if q < HALF:
                b = block(zi, x, c_at(j))
                arrived(allc.at[b, rows_of(q)], c_slot(zi, j, q))
                forward(functools.partial(send, b, q, send_dx, d_slot(zi, j, q), x_peer))
        if q >= HALF:
            b = block(zi, 1 - x, c)
            arrived(allc.at[b, rows_of(q)], x_slot(zi, q))
            for j in range(1, n_cen):
                forward(
                    functools.partial(send, b, q, send_dc, d_slot(zi, n_cen - j, q), c_peer(j))
                )

    def diagonal_step(d, q):
        def visit(zi):
            for j in range(1, n_cen):
                b = block(zi, 1 - x, c_at(j))
                slot = d_slot(zi, j, q)
                up, down = passes_up(zi), passes_down(zi)
                pl.when(jnp.logical_or(up, down))(
                    functools.partial(arrived, allc.at[b, rows_of(q)], slot)
                )
                pl.when(up)(functools.partial(send, b, q, send_dup, slot, up_peer))
                pl.when(down)(functools.partial(send, b, q, send_ddown, slot, down_peer))

        at_distance(d, visit)

    def corner_ready(zi, j):
        b = block(zi, 1 - x, c_at(j))
        for q in range(PIECES):
            seen = passes(zi) if by_line(q) else zi == z
            pl.when(jnp.logical_not(seen))(
                functools.partial(arrived, allc.at[b, rows_of(q)], d_slot(zi, j, q))
            )

    with jax.named_scope("load"):
        load_states.wait()
        load_first.wait()
        load_bias.wait()
        load_cen.start()
    part = n // 2
    for h in range(2):
        rows = pl.ds(h * part, part)
        with jax.named_scope(f"encode{h}"):
            pre = jnp.dot(states_ref[rows, :], first_ref[...], preferred_element_type=jnp.float32)
            hidden = jax.nn.gelu(pre + bias_ref[...][None, :]).astype(jnp.bfloat16)
            if h == 0:
                load_second.wait()
            allc[mine, rows, :] = jnp.dot(
                hidden, second_ref[...], preferred_element_type=jnp.float32
            ).astype(jnp.bfloat16)
        if h == 0:
            with jax.named_scope("barrier"):
                pl.semaphore_wait(barrier, greetings)
        for q in range(h * HALF, (h + 1) * HALF):
            along(z, q)
            aside(z, q)

    def tell(i, peer):
        pl.semaphore_signal(token.at[i], inc=1, device_id=peer, device_id_type=MESH)

    pl.when(z == 0)(lambda: tell(0, up_peer))
    pl.when(z == n_z - 1)(lambda: tell(1, down_peer))

    def pass_on(s):
        @pl.when(jnp.logical_and(has_down, z == s + 1))
        def _():
            pl.semaphore_wait(token.at[0], 1)
            pl.when(has_up)(lambda: tell(0, up_peer))

        @pl.when(jnp.logical_and(has_up, 2 * (n_z - 2 - z) == s))
        def _():
            pl.semaphore_wait(token.at[1], 1)
            pl.when(has_down)(lambda: tell(1, down_peer))

        if s == 2 * (n_z - 2):
            tell(2, x_peer)

    tile = min(512, cen_ref.shape[0])
    tiles = cen_ref.shape[0] // tile
    scale = 2.0 * LOG2E / smoothing_scale

    def tile_rows(i):
        return pl.ds(i * tile, tile) if isinstance(i, int) else pl.ds(pl.multiple_of(i * tile, tile), tile)

    def square_step(i):
        wide = cen_ref[tile_rows(i), :].astype(jnp.float32)
        total = jnp.sum(wide * wide, axis=1, keepdims=True) * (LOG2E / smoothing_scale)
        squares[tile_rows(i), :] = jnp.broadcast_to(total, (tile, 128))

    def less_squares(scores, rows):
        offset = squares[rows, :]
        return jnp.concatenate(
            [scores[:, q * 128:(q + 1) * 128] * scale - offset for q in range(scores.shape[1] // 128)],
            axis=1,
        )

    def stats_step(rows, i, carry):
        peak, total = carry
        scores = lax.dot_general(
            cen_ref[tile_rows(i), :], rows, NT, preferred_element_type=jnp.float32
        )
        scores = less_squares(scores, tile_rows(i)).reshape(tile // 8, 8, rows.shape[0])
        peak_next = jnp.maximum(peak, jnp.max(scores, axis=0))
        total_next = total * jnp.exp2(peak - peak_next) + jnp.sum(
            jnp.exp2(scores - peak_next[None]), axis=0
        )
        return peak_next, total_next

    group_rows = n * n_cen

    def keep_stats(j, first, carry):
        peak, total = carry
        top = jnp.max(peak, axis=0, keepdims=True)
        mass = jnp.sum(total * jnp.exp2(peak - top), axis=0, keepdims=True)
        start = pl.multiple_of(c_at(j) * n + first, 128)
        stat[c, :, pl.ds(start, top.shape[1])] = top
        stat[c, :, pl.ds(group_rows + start, top.shape[1])] = mass

    def fresh(count):
        return jnp.full((8, count), -jnp.inf, jnp.float32), jnp.zeros((8, count), jnp.float32)

    with jax.named_scope("cen"):
        load_cen.wait()
    with jax.named_scope("stats_own"):
        running = fresh(n)
        for i in range(tiles):
            square_step(i)
            running = stats_step(allc[mine], i, running)
        keep_stats(0, 0, running)
    wide = allc[mine].astype(jnp.float32)
    lengths = lax.dot_general(
        jnp.ones((8, width), jnp.float32), wide * wide, NT,
        preferred_element_type=jnp.float32, precision=lax.Precision.HIGHEST,
    )
    weighted[...] = jnp.zeros_like(weighted)
    counts[...] = jnp.zeros_like(counts)

    both = pl.ds(pl.multiple_of((p - core) * n_own, 2 * n_own), 2 * n_own)

    def consume(b, g, ci, count=1, owner=None):
        span = count * n
        rows = allc[pl.ds(b, count)].reshape(span, width)
        pair, seats = both, slice(None)
        if owner is not None:
            pair = pl.ds(pl.multiple_of((p - core + owner) * n_own, n_own), n_own)
            seats = pl.ds(owner, 1)
        scores = lax.dot_general(cen_ref[pair, :], rows, NT, preferred_element_type=jnp.float32)
        level = norm[g, :, pl.ds(pl.multiple_of(ci * n, n), span)]
        resp = jnp.exp2(less_squares(scores, pair) - level)
        lanes = resp[:, 0:128]
        for q in range(1, span // 128):
            lanes = lanes + resp[:, q * 128:(q + 1) * 128]
        counts[seats] += lanes.reshape(-1, n_own, 128)
        weighted[seats] += jnp.dot(
            resp.astype(jnp.bfloat16), rows, preferred_element_type=jnp.float32
        ).reshape(-1, n_own, width)

    def consume_group(g):
        if n_cen <= 2:
            consume(g * n_cen, g, 0, n_cen)
            return

        def one(ci, _):
            consume(g * n_cen + ci, g, ci)
            return 0

        lax.fori_loop(0, n_cen, one, 0)

    def rest_of(b, q, sem):
        arrived(allc.at[b, rows_of(q, HALF)], sem)

    def norm_arrived(zi, xi):
        g = zi * 2 + xi
        arrived(norm.at[g], norm_sem.at[g])

    def line_ready(i):
        zi = ordered(i)
        if i > 0:
            norm_arrived(zi, x)
            for j in range(1, n_cen):
                rest_of(block(zi, x, c_at(j)), HALF, c_rest.at[seat(zi, j)])

    def x_ready(i):
        zi = ordered(i)
        norm_arrived(zi, 1 - x)
        rest_of(block(zi, 1 - x, c), 0, x_rest.at[zi])

    def cross_ready(i):
        x_ready(i)
        for j in range(1, n_cen):
            corner_ready(ordered(i), j)

    def take_line(i):
        consume_group(ordered(i) * 2 + x)

    def take_cross(i):
        consume_group(ordered(i) * 2 + 1 - x)

    def take_last_b(i):
        zi = ordered(i)
        consume(block(zi, 1 - x, c), zi * 2 + 1 - x, c)

    def take_last_d(i, owner):
        zi = ordered(i)
        for j in range(1, n_cen):
            consume(block(zi, 1 - x, c_at(j)), zi * 2 + 1 - x, c_at(j), owner=owner)

    def cross_stats(j, first):
        b = block(z, x, c_at(j))

        def step(i, carry):
            return stats_step(allc[b, pl.ds(first, n // 2), :], i, carry)

        running = fresh(n // 2)
        if n_cen <= 2:
            for i in range(tiles):
                running = step(i, running)
        else:
            running = lax.fori_loop(0, tiles, step, running)
        keep_stats(j, first, running)

    def share_stats():
        for j in range(1, n_cen):
            remote(
                stat.at[c], stat.at[c], send_stat, stat_sem.at[n_cen - j - 1], c_peer(j)
            ).start()

    def share_norm():
        for j in range(1, n_cen):
            s = c_at(j)
            arrived(stat.at[s], stat_sem.at[j - 1])
        top = stat[0, :, 0:group_rows]
        for s in range(1, n_cen):
            top = jnp.maximum(top, stat[s, :, 0:group_rows])
        mass = jnp.zeros_like(top)
        for s in range(n_cen):
            mass = mass + stat[s, :, group_rows:2 * group_rows] * jnp.exp2(
                stat[s, :, 0:group_rows] - top
            )
        level = top + jnp.log(mass) * LOG2E
        g = z * 2 + x
        norm[g] = level
        pl.semaphore_wait(token.at[2], 1)
        for k in range(1, 2 * n_z):
            h = lax.rem(g + k, 2 * n_z)
            remote(norm.at[g], norm.at[g], send_norm, norm_sem.at[g], at(h // 2, lax.rem(h, 2), c)).start()
        own = norm[g, :, pl.ds(pl.multiple_of(c * n, n), n)]
        pen_ref[...] = (-(smoothing_scale / width)) * (
            own * math.log(2.0) - lengths[0:1, :] / smoothing_scale
        )

    total_steps = n_z * PIECES
    norm_at, early_at = 2 * PIECES - 1, (n_z - 1) * PIECES - 1

    diagonals = {}
    for q in range(PIECES):
        diagonals.setdefault(min(PIECES + 1 + (q + 1) // 2, total_steps - 1), []).append((0, q))
    for d in range(1, n_z):
        for e in range(2):
            s = min(PIECES + 2 + 3 * d + e, total_steps - 1)
            diagonals.setdefault(s, []).append((d, HALF - 1 + e))
    for s in range(total_steps):
        i, q = 1 + s // PIECES, s % PIECES
        with jax.named_scope(f"move{s}"):
            if i < n_z:
                if i == 1:
                    line_forward(1, q)
                line_step(i, q)
                aside(ordered(i), q)
                if i > 1 and q < 2:
                    for ahead in range(PIECES - 1) if q == 0 else (PIECES - 1,):
                        line_forward(i, ahead)
            cross_step(i - 1, q)
            for d, piece_index in diagonals.get(s, ()):
                diagonal_step(d, piece_index)
            if s <= max(n_z - 2, 2 * (n_z - 2)):
                pass_on(s)
        with jax.named_scope(f"work{s}"):
            if s == PIECES - 1:
                for j in range(1, n_cen):
                    cross_stats(j, 0)
                    rest_of(block(z, x, c_at(j)), HALF, c_rest.at[seat(z, j)])
                    cross_stats(j, n // 2)
                share_stats()
            if s == norm_at:
                share_norm()
                take_line(0)
            if s == early_at:
                line_ready(1)
                take_line(1)
    with jax.named_scope("tail"):
        last = n_z - 1
        cross_ready(0)
        for i in range(2, n_z):
            line_ready(i)
            if i < last:
                cross_ready(i - 1)
                take_cross(i - 2)
                take_line(i)
        cross_ready(last - 1)
        x_ready(last)
        take_cross(last - 2)
        take_line(last)
        take_cross(last - 1)
        take_last_b(last)
    with jax.named_scope("tail_d"):
        for j in range(1, n_cen):
            corner_ready(ordered(last), j)
        take_last_d(last, 1 - core)

    with jax.named_scope("pair"):
        sums = remote(
            weighted.at[1 - core], other_sums, send_pair.at[0], pair_sem.at[0], core_peer
        )
        tally = remote(
            counts.at[1 - core], other_counts, send_pair.at[1], pair_sem.at[1], core_peer
        )
        tally.start()
        sums.start()
        take_last_d(last, core)
        own_rows = pl.ds(pl.multiple_of(p * n_own, n_own), n_own)
        tally.wait()
        share = 1.0 / (
            jnp.sum(counts[core] + other_counts[...], axis=1, keepdims=True) + 1.0
        )
        sums.wait()
    with jax.named_scope("final"):
        out_ref[...] = (
            weighted[core] + other_sums[...] + cen_ref[own_rows, :].astype(jnp.float32)
        ) * share

    with jax.named_scope("sent"):

        def left(ref, send_sem):
            remote(ref, ref, send_sem, pair_sem.at[0], core_peer).wait_send()

        left(allc.at[pl.ds(0, n_z)], send_x)
        left(allc.at[pl.ds(0, others * n_z)], send_c)

        def left_corner(near):
            corner = others * (HALF + (n_z - 1 - near) * (HALF - 1))
            left(allc.at[pl.ds(0, corner), rows_of(0)], send_dx)
            left(allc.at[pl.ds(0, corner), rows_of(0)], send_dc)

        inside = jnp.logical_and(has_up, has_down)
        pl.when(inside)(lambda: left_corner(2))
        pl.when(jnp.logical_not(inside))(lambda: left_corner(1))

        def left_line(count, whole, parts):
            left(allc.at[pl.ds(0, count)], whole)
            left(allc.at[pl.ds(0, (count + 1) * others), rows_of(0, 2)], parts)

        for zi in range(n_z - 1):
            pl.when(z == zi)(functools.partial(left_line, zi + 1, send_up, send_dup))
            pl.when(z == n_z - 1 - zi)(
                functools.partial(left_line, zi + 1, send_down, send_ddown)
            )
        left(stat.at[pl.ds(0, others)], send_stat)
        left(norm.at[pl.ds(0, 2 * n_z - 1)], send_norm)


def finish(fresh_ref, pen_ref, out_ref, cost_ref):
    out_ref[0] = fresh_ref[...]
    cost_ref[...] = pen_ref[0]


def body(n_pts, n_cen, states, first_weight, first_bias, second_weight, centroids):
    n, width = states.shape[0], second_weight.shape[1]
    k_dev = centroids.shape[1]
    owned = k_dev // n_pts
    n_z, others = n_pts // 4, n_cen - 1
    dma = pltpu.SemaphoreType.DMA
    vmem, f32 = pltpu.VMEM, jnp.float32
    args = [
        pltpu.with_memory_space_constraint(v, pltpu.HBM)
        for v in (states, first_weight, first_bias, second_weight, centroids)
    ]
    fresh, penalty = pl.pallas_call(
        functools.partial(kernel, n_pts, n_cen),
        out_shape=(vmem((owned, width), f32), vmem((1, n), f32)),
        in_specs=[pl.BlockSpec(memory_space=pltpu.HBM)] * 5,
        out_specs=(pl.BlockSpec(memory_space=vmem),) * 2,
        scratch_shapes=[
            vmem(states.shape, states.dtype),
            vmem(first_weight.shape, first_weight.dtype),
            vmem(first_bias.shape, first_bias.dtype),
            vmem(second_weight.shape, second_weight.dtype),
            vmem(centroids.shape[1:], centroids.dtype),
            dma((5,)),
            vmem((2 * n_z * n_cen, n, width), jnp.bfloat16),
            vmem((n_cen, 1, 2 * n_cen * n), f32),
            vmem((2 * n_z, 1, n_cen * n), f32),
            vmem((k_dev, 128), f32),
            vmem((2, owned, width), f32),
            vmem((2, owned, 128), f32),
            vmem((owned, width), f32),
            vmem((owned, 128), f32),
            dma((n_z, PIECES)),
            dma((n_z * others, HALF)),
            dma((n_z * others,)),
            dma((n_z, HALF)),
            dma((n_z,)),
            dma((n_z * others, PIECES)),
            dma((others,)),
            dma((2 * n_z,)),
            dma((2,)),
            *([dma] * 10),
            dma((2,)),
            pltpu.SemaphoreType.REGULAR((3,)),
        ],
        compiler_params=pltpu.CompilerParams(
            collective_id=0, has_side_effects=True, vmem_limit_bytes=48 * 1024 * 1024
        ),
    )(*args)
    return pl.pallas_call(
        finish,
        out_shape=(
            jax.ShapeDtypeStruct((1, owned, width), f32),
            jax.ShapeDtypeStruct((n,), f32),
        ),
        in_specs=[pl.BlockSpec(memory_space=vmem)] * 2,
        out_specs=(pl.BlockSpec(memory_space=vmem),) * 2,
        compiler_params=pltpu.CompilerParams(vmem_limit_bytes=4 * 1024 * 1024),
    )(fresh, penalty)


def solution(mesh):
    placed = (P(("pts", "cen"), None), P(), P(), P(), P("cen", None, None))
    return jax.shard_map(
        functools.partial(body, mesh.shape["pts"], mesh.shape["cen"]),
        mesh=mesh,
        in_specs=placed,
        out_specs=(P("cen", "pts", None), P(("pts", "cen"))),
        check_vma=False,
    )
```

```python
import functools
import math

import jax
import jax.numpy as jnp
from jax import lax
from jax.experimental import pallas as pl
from jax.experimental.pallas import tpu as pltpu
from jax.sharding import PartitionSpec as P

smoothing_scale = 16.0
LOG2E = math.log2(math.e)
MESH = pl.DeviceIdType.MESH
NT = (((1,), (1,)), ((), ()))
PIECES = 4
HALF = PIECES // 2
LINE_PIECES = (0, HALF)
ORDER = (1, 0, 3, 2)


def kernel(
    n_pts, n_cen, states_hbm, first_hbm, bias_hbm, second_hbm, cen_hbm, out_ref, pen_ref,
    states_ref, first_ref, bias_ref, second_ref, cen_ref,
    allc, stat, norm, squares, weighted, counts, other_sums, other_counts,
    line_sem, c_sem, c_rest, x_sem, x_rest, d_sem, stat_sem, norm_sem,
    send_up, send_down, send_x, send_c, send_dup, send_ddown, send_dx, send_dc,
    send_stat, send_norm, token,
):
    n, width = states_ref.shape[0], second_ref.shape[1]
    n_z, others = n_pts // 4, n_cen - 1
    n_own = out_ref.shape[0]
    piece = n // PIECES

    def load(i, src, dst):
        return pltpu.make_async_copy(src, dst, (send_x, send_c, send_dx, send_dc, send_stat)[i])

    load_states = load(0, states_hbm, states_ref)
    load_first = load(1, first_hbm, first_ref)
    load_bias = load(2, bias_hbm, bias_ref)
    load_second = load(3, second_hbm, second_ref)
    load_cen = load(4, cen_hbm.at[0], cen_ref)
    def start(i, src, dst, parts):
        rows = dst.shape[0] // parts
        for k in range(parts):
            at_rows = pl.ds(k * rows, rows)
            load(i, src.at[at_rows], dst.at[at_rows]).start()

    start(0, states_hbm, states_ref, 1)
    start(1, first_hbm, first_ref, 4)
    load_bias.start()
    start(3, second_hbm, second_ref, 2)

    p, c = lax.axis_index("pts"), lax.axis_index("cen")
    core, x, z = lax.rem(p, 2), lax.rem(p // 2, 2), p // 4
    has_up, has_down = z < n_z - 1, z > 0

    side = lax.rem(core + x + z + c, 2)

    def at(zi, xi, ci):
        return ((zi * 2 + xi) * 2 + lax.rem(side + xi + zi + ci, 2), ci)

    def c_at(j):
        return lax.rem(c + j, n_cen)

    def block(zi, xi, ci):
        return (zi * 2 + xi) * n_cen + ci

    def c_peer(j):
        return at(z, x, c_at(j))

    up_peer, down_peer = at(lax.rem(z + 1, n_z), x, c), at(lax.rem(z + n_z - 1, n_z), x, c)
    x_peer, core_peer = at(z, 1 - x, c), (p + 1 - 2 * core, c)
    mine = block(z, x, c)

    barrier = pltpu.get_barrier_semaphore()

    def greet(peer):
        pl.semaphore_signal(barrier, inc=1, device_id=peer, device_id_type=MESH)

    pl.when(has_up)(lambda: greet(up_peer))
    pl.when(has_down)(lambda: greet(down_peer))
    greet(x_peer)
    greet(core_peer)
    for j in range(1, n_cen):
        greet(c_peer(j))
    greetings = 2 + others + has_up.astype(jnp.int32) + has_down.astype(jnp.int32)

    def rows_of(q, count=1):
        return pl.ds(q * piece, count * piece)

    def remote(src, dst, send, recv, peer):
        return pltpu.make_async_remote_copy(
            src_ref=src, dst_ref=dst, send_sem=send, recv_sem=recv,
            device_id=peer, device_id_type=MESH,
        )

    def send(b, q, send_sem, recv_sem, peer):
        ref = allc.at[b, rows_of(q)]
        remote(ref, ref, send_sem, recv_sem, peer).start()

    def arrived(ref, recv_sem):
        remote(ref, ref, send_x, recv_sem, core_peer).wait_recv()

    def seat(zi, j):
        return zi * others + j - 1

    def c_slot(zi, j, q):
        return c_sem.at[seat(zi, j), q] if q < HALF else c_rest.at[seat(zi, j)]

    def x_slot(zi, q):
        return x_rest.at[zi] if q < HALF else x_sem.at[zi, q - HALF]

    def at_distance(d, visit):
        if d == 0:
            visit(z)
            return
        pl.when(z + d < n_z)(lambda: visit(z + d))
        pl.when(z >= d)(lambda: visit(z - d))

    def along(zi, q):
        b = block(zi, x, c)
        pl.when(passes_up(zi))(lambda: send(b, q, send_up, line_sem.at[zi, q], up_peer))
        pl.when(passes_down(zi))(lambda: send(b, q, send_down, line_sem.at[zi, q], down_peer))

    def aside(zi, q):
        b = block(zi, x, c)
        for j in range(1, n_cen):
            send(b, q, send_c, c_slot(zi, n_cen - j, q), c_peer(j))
        send(b, q, send_x, x_slot(zi, q), x_peer)

    def passes_up(zi):
        return jnp.logical_and(has_up, zi <= z)

    def passes_down(zi):
        return jnp.logical_and(has_down, zi >= z)

    def passes(zi):
        return jnp.logical_or(passes_up(zi), passes_down(zi))

    def line_arrived(zi, q):
        arrived(allc.at[block(zi, x, c), rows_of(q)], line_sem.at[zi, q])

    def line_forward(d, q):
        def visit(zi):
            @pl.when(passes(zi))
            def _():
                line_arrived(zi, q)
                along(zi, q)

        at_distance(d, visit)

    def line_step(i, q):
        zi = ordered(i)
        pl.when(jnp.logical_not(passes(zi)))(lambda: line_arrived(zi, q))

    def ordered(i):
        near = jnp.minimum(z, n_z - 1 - z)
        beside = z + (i + 1) // 2 if i % 2 else z - i // 2
        beyond = jnp.where(z <= n_z - 1 - z, i, n_z - 1 - i)
        return jnp.where(i <= 2 * near, beside, beyond)

    def d_slot(zi, j, q):
        return d_sem.at[seat(zi, j), q]

    def by_line(q):
        return q in LINE_PIECES

    def cross_step(i, q):
        zi = ordered(i)

        def forward(visit):
            if i == 0:
                visit()
            elif not by_line(q):
                pl.when(jnp.abs(zi - z) > 1)(visit)

        for j in range(1, n_cen):
            if q < HALF:
                b = block(zi, x, c_at(j))
                arrived(allc.at[b, rows_of(q)], c_slot(zi, j, q))
                forward(functools.partial(send, b, q, send_dx, d_slot(zi, j, q), x_peer))
        if q >= HALF:
            b = block(zi, 1 - x, c)
            arrived(allc.at[b, rows_of(q)], x_slot(zi, q))
            for j in range(1, n_cen):
                forward(
                    functools.partial(send, b, q, send_dc, d_slot(zi, n_cen - j, q), c_peer(j))
                )

    def diagonal_step(d, q):
        def visit(zi):
            for j in range(1, n_cen):
                b = block(zi, 1 - x, c_at(j))
                slot = d_slot(zi, j, q)
                up, down = passes_up(zi), passes_down(zi)
                pl.when(jnp.logical_or(up, down))(
                    functools.partial(arrived, allc.at[b, rows_of(q)], slot)
                )
                pl.when(up)(functools.partial(send, b, q, send_dup, slot, up_peer))
                pl.when(down)(functools.partial(send, b, q, send_ddown, slot, down_peer))

        at_distance(d, visit)

    def corner_ready(zi, j):
        b = block(zi, 1 - x, c_at(j))
        for q in range(PIECES):
            seen = passes(zi) if by_line(q) else zi == z
            pl.when(jnp.logical_not(seen))(
                functools.partial(arrived, allc.at[b, rows_of(q)], d_slot(zi, j, q))
            )

    with jax.named_scope("load"):
        load_states.wait()
        load_first.wait()
        load_bias.wait()
        load_cen.start()
    part = n // 2
    for h in range(2):
        rows = pl.ds(h * part, part)
        with jax.named_scope(f"encode{h}"):
            pre = jnp.dot(states_ref[rows, :], first_ref[...], preferred_element_type=jnp.float32)
            hidden = jax.nn.gelu(pre + bias_ref[...][None, :]).astype(jnp.bfloat16)
            if h == 0:
                load_second.wait()
            allc[mine, rows, :] = jnp.dot(
                hidden, second_ref[...], preferred_element_type=jnp.float32
            ).astype(jnp.bfloat16)
        if h == 0:
            with jax.named_scope("barrier"):
                pl.semaphore_wait(barrier, greetings)
        for q in range(h * HALF, (h + 1) * HALF):
            along(z, ORDER[q])
            aside(z, q)

    def tell(i, peer):
        pl.semaphore_signal(token.at[i], inc=1, device_id=peer, device_id_type=MESH)

    pl.when(z == 0)(lambda: tell(0, up_peer))
    pl.when(z == n_z - 1)(lambda: tell(1, down_peer))

    def pass_on(s):
        @pl.when(jnp.logical_and(has_down, z == s + 1))
        def _():
            pl.semaphore_wait(token.at[0], 1)
            pl.when(has_up)(lambda: tell(0, up_peer))

        @pl.when(jnp.logical_and(has_up, 2 * (n_z - 2 - z) == s))
        def _():
            pl.semaphore_wait(token.at[1], 1)
            pl.when(has_down)(lambda: tell(1, down_peer))

        if s == 2 * (n_z - 2):
            tell(2, x_peer)

    tile = min(512, cen_ref.shape[0])
    tiles = cen_ref.shape[0] // tile
    scale = 2.0 * LOG2E / smoothing_scale

    def tile_rows(i):
        return pl.ds(i * tile, tile) if isinstance(i, int) else pl.ds(pl.multiple_of(i * tile, tile), tile)

    def square_step(i):
        wide = cen_ref[tile_rows(i), :].astype(jnp.float32)
        total = jnp.sum(wide * wide, axis=1, keepdims=True) * (LOG2E / smoothing_scale)
        squares[tile_rows(i), :] = jnp.broadcast_to(total, (tile, 128))

    def less_squares(scores, rows):
        offset = squares[rows, :]
        return jnp.concatenate(
            [scores[:, q * 128:(q + 1) * 128] * scale - offset for q in range(scores.shape[1] // 128)],
            axis=1,
        )

    def stats_step(rows, i, carry):
        peak, total = carry
        scores = lax.dot_general(
            cen_ref[tile_rows(i), :], rows, NT, preferred_element_type=jnp.float32
        )
        scores = less_squares(scores, tile_rows(i)).reshape(tile // 8, 8, rows.shape[0])
        peak_next = jnp.maximum(peak, jnp.max(scores, axis=0))
        total_next = total * jnp.exp2(peak - peak_next) + jnp.sum(
            jnp.exp2(scores - peak_next[None]), axis=0
        )
        return peak_next, total_next

    group_rows = n * n_cen

    def keep_stats(j, carry):
        peak, total = carry
        top = jnp.max(peak, axis=0, keepdims=True)
        mass = jnp.sum(total * jnp.exp2(peak - top), axis=0, keepdims=True)
        start = pl.multiple_of(c_at(j) * n, n)
        stat[c, :, pl.ds(start, top.shape[1])] = top
        stat[c, :, pl.ds(group_rows + start, top.shape[1])] = mass

    def fresh(count):
        return jnp.full((8, count), -jnp.inf, jnp.float32), jnp.zeros((8, count), jnp.float32)

    with jax.named_scope("cen"):
        load_cen.wait()
    with jax.named_scope("stats_own"):
        running = fresh(n)
        for i in range(tiles):
            square_step(i)
            running = stats_step(allc[mine], i, running)
        keep_stats(0, running)
    wide = allc[mine].astype(jnp.float32)
    lengths = lax.dot_general(
        jnp.ones((8, width), jnp.float32), wide * wide, NT,
        preferred_element_type=jnp.float32, precision=lax.Precision.HIGHEST,
    )
    weighted[...] = jnp.zeros_like(weighted)
    counts[...] = jnp.zeros_like(counts)

    both = pl.ds(pl.multiple_of((p - core) * n_own, 2 * n_own), 2 * n_own)

    def consume(b, g, ci, count=1, owner=None):
        span = count * n
        rows = allc[pl.ds(b, count)].reshape(span, width)
        pair, seats = both, slice(None)
        if owner is not None:
            pair = pl.ds(pl.multiple_of((p - core + owner) * n_own, n_own), n_own)
            seats = pl.ds(owner, 1)
        scores = lax.dot_general(cen_ref[pair, :], rows, NT, preferred_element_type=jnp.float32)
        level = norm[g, :, pl.ds(pl.multiple_of(ci * n, n), span)]
        resp = jnp.exp2(less_squares(scores, pair) - level)
        lanes = resp[:, 0:128]
        for q in range(1, span // 128):
            lanes = lanes + resp[:, q * 128:(q + 1) * 128]
        counts[seats] += lanes.reshape(-1, n_own, 128)
        weighted[seats] += jnp.dot(
            resp.astype(jnp.bfloat16), rows, preferred_element_type=jnp.float32
        ).reshape(-1, n_own, width)

    def consume_group(g, owner=None):
        if n_cen <= 2:
            consume(g * n_cen, g, 0, n_cen, owner=owner)
            return

        def one(ci, _):
            consume(g * n_cen + ci, g, ci, owner=owner)
            return 0

        lax.fori_loop(0, n_cen, one, 0)

    def rest_of(b, q, sem):
        arrived(allc.at[b, rows_of(q, HALF)], sem)

    def norm_arrived(zi, xi):
        g = zi * 2 + xi
        arrived(norm.at[g], norm_sem.at[g])

    def line_ready(i):
        zi = ordered(i)
        if i > 0:
            norm_arrived(zi, x)
            for j in range(1, n_cen):
                b = block(zi, x, c_at(j))
                for q in range(HALF):
                    if by_line(q):
                        arrived(allc.at[b, rows_of(q)], c_slot(zi, j, q))
                rest_of(b, HALF, c_rest.at[seat(zi, j)])

    def x_ready(i):
        zi = ordered(i)
        norm_arrived(zi, 1 - x)
        b = block(zi, 1 - x, c)
        rest_of(b, 0, x_rest.at[zi])
        if i > 0:
            for q in range(HALF, PIECES):
                if by_line(q):
                    arrived(allc.at[b, rows_of(q)], x_slot(zi, q))

    def cross_ready(i):
        x_ready(i)
        for j in range(1, n_cen):
            corner_ready(ordered(i), j)

    def take_line(i, owner=None):
        consume_group(ordered(i) * 2 + x, owner)

    def take_cross(i, owner=None):
        consume_group(ordered(i) * 2 + 1 - x, owner)

    def take_last_b(i, owner):
        zi = ordered(i)
        consume(block(zi, 1 - x, c), zi * 2 + 1 - x, c, owner=owner)

    def take_last_d(i, owner):
        zi = ordered(i)
        for j in range(1, n_cen):
            consume(block(zi, 1 - x, c_at(j)), zi * 2 + 1 - x, c_at(j), owner=owner)

    def cross_stats(j):
        b = block(z, x, c_at(j))

        def step(i, carry):
            return stats_step(allc[b], i, carry)

        running = fresh(n)
        if n_cen <= 2:
            for i in range(tiles):
                running = step(i, running)
        else:
            running = lax.fori_loop(0, tiles, step, running)
        keep_stats(j, running)

    def share_stats():
        for j in range(1, n_cen):
            remote(
                stat.at[c], stat.at[c], send_stat, stat_sem.at[n_cen - j - 1], c_peer(j)
            ).start()

    def share_norm():
        for j in range(1, n_cen):
            s = c_at(j)
            arrived(stat.at[s], stat_sem.at[j - 1])
        top = stat[0, :, 0:group_rows]
        for s in range(1, n_cen):
            top = jnp.maximum(top, stat[s, :, 0:group_rows])
        mass = jnp.zeros_like(top)
        for s in range(n_cen):
            mass = mass + stat[s, :, group_rows:2 * group_rows] * jnp.exp2(
                stat[s, :, 0:group_rows] - top
            )
        level = top + jnp.log(mass) * LOG2E
        g = z * 2 + x
        norm[g] = level
        pl.semaphore_wait(token.at[2], 1)
        for k in range(1, 2 * n_z):
            h = lax.rem(g + k, 2 * n_z)
            remote(norm.at[g], norm.at[g], send_norm, norm_sem.at[g], at(h // 2, lax.rem(h, 2), c)).start()
        own = norm[g, :, pl.ds(pl.multiple_of(c * n, n), n)]
        pen_ref[...] = (-(smoothing_scale / width)) * (
            own * math.log(2.0) - lengths[0:1, :] / smoothing_scale
        )

    total_steps = n_z * PIECES
    norm_at = 2 * PIECES - 1

    diagonals = {}
    for q, s in enumerate((1, 3, 2, 3)):
        diagonals.setdefault(min(PIECES + s, total_steps - 1), []).append((0, q))
    for d in range(1, n_z):
        for e in range(2):
            s = min(2 * PIECES + 1 + 3 * (d - 1) + e, total_steps - 1)
            diagonals.setdefault(s, []).append((d, LINE_PIECES[e]))
    for s in range(total_steps):
        i, q = 1 + s // PIECES, s % PIECES
        with jax.named_scope(f"move{s}"):
            if i < n_z:
                if i == 1:
                    line_forward(1, ORDER[q])
                line_step(i, ORDER[q])
                if i == 1:
                    cross_step(0, q)
                aside(ordered(i), ORDER[q])
                if i > 1 and q < 2:
                    for ahead in ORDER[:-1] if q == 0 else ORDER[-1:]:
                        line_forward(i, ahead)
            if i > 1 and q % 2 == 0:
                cross_step(i - 1, q + 1)
            for d, piece_index in diagonals.get(s, ()):
                diagonal_step(d, piece_index)
            if s <= max(n_z - 2, 2 * (n_z - 2)):
                pass_on(s)
        with jax.named_scope(f"work{s}"):
            if s == PIECES - 1:
                for j in range(1, n_cen):
                    rest_of(block(z, x, c_at(j)), HALF, c_rest.at[seat(z, j)])
                    cross_stats(j)
                share_stats()
            if s == norm_at:
                share_norm()
                take_line(0)
    last = n_z - 1
    takes = []
    for i in range(1, n_z):
        takes += [
            (functools.partial(line_ready, i), functools.partial(take_line, i)),
            (functools.partial(cross_ready, i - 1), functools.partial(take_cross, i - 1)),
        ]
    takes.append((functools.partial(x_ready, last), functools.partial(take_last_b, last)))
    ahead = 2
    with jax.named_scope("tail"):
        for first in range(0, len(takes), 2):
            for ready, _ in takes[first:first + 2]:
                ready()
            for _, take in takes[first:first + 2]:
                take(owner=1 - core)
        for _, take in takes[:ahead]:
            take(owner=core)
    with jax.named_scope("sent"):

        def left(ref, send_sem):
            remote(ref, ref, send_sem, line_sem.at[z, 0], core_peer).wait_send()

        left(allc.at[pl.ds(0, n_z)], send_x)
        left(allc.at[pl.ds(0, others * n_z)], send_c)

        def left_corner(near):
            corner = others * (HALF + (n_z - 1 - near) * (HALF - 1))
            left(allc.at[pl.ds(0, corner), rows_of(0)], send_dx)
            left(allc.at[pl.ds(0, corner), rows_of(0)], send_dc)

        inside = jnp.logical_and(has_up, has_down)
        pl.when(inside)(lambda: left_corner(2))
        pl.when(jnp.logical_not(inside))(lambda: left_corner(1))

        def left_line(count, whole, parts):
            left(allc.at[pl.ds(0, count)], whole)
            left(allc.at[pl.ds(0, (count + 1) * others), rows_of(0, 2)], parts)

        for zi in range(n_z - 1):
            pl.when(z == zi)(functools.partial(left_line, zi + 1, send_up, send_dup))
            pl.when(z == n_z - 1 - zi)(
                functools.partial(left_line, zi + 1, send_down, send_ddown)
            )
        left(stat.at[pl.ds(0, others)], send_stat)
        left(norm.at[pl.ds(0, 2 * n_z - 1)], send_norm)

    with jax.named_scope("tail_d"):
        for j in range(1, n_cen):
            corner_ready(ordered(last), j)
        take_last_d(last, 1 - core)

    with jax.named_scope("pair"):
        sums = remote(
            weighted.at[1 - core], other_sums, send_x, line_sem.at[z, 0], core_peer
        )
        tally = remote(
            counts.at[1 - core], other_counts, send_c, line_sem.at[z, 1], core_peer
        )
        tally.start()
        sums.start()
        for _, take in takes[ahead:]:
            take(owner=core)
        take_last_d(last, core)
        own_rows = pl.ds(pl.multiple_of(p * n_own, n_own), n_own)
        tally.wait()
        share = 1.0 / (
            jnp.sum(counts[core] + other_counts[...], axis=1, keepdims=True) + 1.0
        )
        sums.wait()
    with jax.named_scope("final"):
        out_ref[...] = (
            weighted[core] + other_sums[...] + cen_ref[own_rows, :].astype(jnp.float32)
        ) * share


def finish(fresh_ref, pen_ref, out_ref, cost_ref):
    out_ref[0] = fresh_ref[...]
    cost_ref[...] = pen_ref[0]


def body(n_pts, n_cen, states, first_weight, first_bias, second_weight, centroids):
    n, width = states.shape[0], second_weight.shape[1]
    k_dev = centroids.shape[1]
    owned = k_dev // n_pts
    n_z, others = n_pts // 4, n_cen - 1
    dma = pltpu.SemaphoreType.DMA
    vmem, f32 = pltpu.VMEM, jnp.float32
    args = [
        pltpu.with_memory_space_constraint(v, pltpu.HBM)
        for v in (states, first_weight, first_bias, second_weight, centroids)
    ]
    fresh, penalty = pl.pallas_call(
        functools.partial(kernel, n_pts, n_cen),
        out_shape=(vmem((owned, width), f32), vmem((1, n), f32)),
        in_specs=[pl.BlockSpec(memory_space=pltpu.HBM)] * 5,
        out_specs=(pl.BlockSpec(memory_space=vmem),) * 2,
        scratch_shapes=[
            vmem(states.shape, states.dtype),
            vmem(first_weight.shape, first_weight.dtype),
            vmem(first_bias.shape, first_bias.dtype),
            vmem(second_weight.shape, second_weight.dtype),
            vmem(centroids.shape[1:], centroids.dtype),
            vmem((2 * n_z * n_cen, n, width), jnp.bfloat16),
            vmem((n_cen, 1, 2 * n_cen * n), f32),
            vmem((2 * n_z, 1, n_cen * n), f32),
            vmem((k_dev, 128), f32),
            vmem((2, owned, width), f32),
            vmem((2, owned, 128), f32),
            vmem((owned, width), f32),
            vmem((owned, 128), f32),
            dma((n_z, PIECES)),
            dma((n_z * others, HALF)),
            dma((n_z * others,)),
            dma((n_z, HALF)),
            dma((n_z,)),
            dma((n_z * others, PIECES)),
            dma((others,)),
            dma((2 * n_z,)),
            *([dma] * 10),
            pltpu.SemaphoreType.REGULAR((3,)),
        ],
        compiler_params=pltpu.CompilerParams(
            collective_id=0, has_side_effects=True, vmem_limit_bytes=48 * 1024 * 1024
        ),
    )(*args)
    return pl.pallas_call(
        finish,
        out_shape=(
            jax.ShapeDtypeStruct((1, owned, width), f32),
            jax.ShapeDtypeStruct((n,), f32),
        ),
        in_specs=[pl.BlockSpec(memory_space=vmem)] * 2,
        out_specs=(pl.BlockSpec(memory_space=vmem),) * 2,
        compiler_params=pltpu.CompilerParams(vmem_limit_bytes=4 * 1024 * 1024),
    )(fresh, penalty)


def solution(mesh):
    placed = (P(("pts", "cen"), None), P(), P(), P(), P("cen", None, None))
    return jax.shard_map(
        functools.partial(body, mesh.shape["pts"], mesh.shape["cen"]),
        mesh=mesh,
        in_specs=placed,
        out_specs=(P("cen", "pts", None), P(("pts", "cen"))),
        check_vma=False,
    )
```

```python
import functools
import math

import jax
import jax.numpy as jnp
from jax import lax
from jax.experimental import pallas as pl
from jax.experimental.pallas import tpu as pltpu
from jax.sharding import PartitionSpec as P

smoothing_scale = 16.0
LOG2E = math.log2(math.e)
MESH = pl.DeviceIdType.MESH
NT = (((1,), (1,)), ((), ()))
PIECES = 4
HALF = PIECES // 2
LINE_PIECES = (0, HALF)
ORDER = (1, 0, 3, 2)


def kernel(
    n_pts, n_cen, states_hbm, first_hbm, bias_hbm, second_hbm, cen_hbm, out_ref, pen_ref,
    states_ref, first_ref, bias_ref, second_ref, cen_ref,
    allc, stat, norm, squares, weighted, counts, other_sums, other_counts,
    line_sem, c_sem, c_rest, x_sem, x_rest, d_sem, stat_sem, norm_sem,
    send_up, send_down, send_x, send_c, send_dup, send_ddown, send_dx, send_dc,
    send_stat, send_norm, token,
):
    n, width = states_ref.shape[0], second_ref.shape[1]
    n_z, others = n_pts // 4, n_cen - 1
    n_own = out_ref.shape[0]
    piece = n // PIECES

    def load(i, src, dst):
        return pltpu.make_async_copy(src, dst, (send_x, send_c, send_dx, send_dc, send_stat)[i])

    load_states = load(0, states_hbm, states_ref)
    load_first = load(1, first_hbm, first_ref)
    load_bias = load(2, bias_hbm, bias_ref)
    load_second = load(3, second_hbm, second_ref)
    load_cen = load(4, cen_hbm.at[0], cen_ref)
    def start(i, src, dst, parts):
        rows = dst.shape[0] // parts
        for k in range(parts):
            at_rows = pl.ds(k * rows, rows)
            load(i, src.at[at_rows], dst.at[at_rows]).start()

    start(0, states_hbm, states_ref, 1)
    start(1, first_hbm, first_ref, 4)
    load_bias.start()
    start(3, second_hbm, second_ref, 2)

    p, c = lax.axis_index("pts"), lax.axis_index("cen")
    core, x, z = lax.rem(p, 2), lax.rem(p // 2, 2), p // 4
    has_up, has_down = z < n_z - 1, z > 0

    side = lax.rem(core + x + z + c, 2)

    def at(zi, xi, ci):
        return ((zi * 2 + xi) * 2 + lax.rem(side + xi + zi + ci, 2), ci)

    def c_at(j):
        return lax.rem(c + j, n_cen)

    def block(zi, xi, ci):
        return (zi * 2 + xi) * n_cen + ci

    def c_peer(j):
        return at(z, x, c_at(j))

    up_peer, down_peer = at(lax.rem(z + 1, n_z), x, c), at(lax.rem(z + n_z - 1, n_z), x, c)
    x_peer, core_peer = at(z, 1 - x, c), (p + 1 - 2 * core, c)
    mine = block(z, x, c)

    barrier = pltpu.get_barrier_semaphore()

    def greet(peer):
        pl.semaphore_signal(barrier, inc=1, device_id=peer, device_id_type=MESH)

    pl.when(has_up)(lambda: greet(up_peer))
    pl.when(has_down)(lambda: greet(down_peer))
    greet(x_peer)
    greet(core_peer)
    for j in range(1, n_cen):
        greet(c_peer(j))
    greetings = 2 + others + has_up.astype(jnp.int32) + has_down.astype(jnp.int32)

    def rows_of(q, count=1):
        return pl.ds(q * piece, count * piece)

    def remote(src, dst, send, recv, peer):
        return pltpu.make_async_remote_copy(
            src_ref=src, dst_ref=dst, send_sem=send, recv_sem=recv,
            device_id=peer, device_id_type=MESH,
        )

    def send(b, q, send_sem, recv_sem, peer):
        ref = allc.at[b, rows_of(q)]
        remote(ref, ref, send_sem, recv_sem, peer).start()

    def arrived(ref, recv_sem):
        remote(ref, ref, send_x, recv_sem, core_peer).wait_recv()

    def seat(zi, j):
        return zi * others + j - 1

    def c_slot(zi, j, q):
        return c_sem.at[seat(zi, j), q] if q < HALF else c_rest.at[seat(zi, j)]

    def x_slot(zi, q):
        return x_rest.at[zi] if q < HALF else x_sem.at[zi, q - HALF]

    def at_distance(d, visit):
        if d == 0:
            visit(z)
            return
        pl.when(z + d < n_z)(lambda: visit(z + d))
        pl.when(z >= d)(lambda: visit(z - d))

    def along(zi, q):
        b = block(zi, x, c)
        pl.when(passes_up(zi))(lambda: send(b, q, send_up, line_sem.at[zi, q], up_peer))
        pl.when(passes_down(zi))(lambda: send(b, q, send_down, line_sem.at[zi, q], down_peer))

    def aside(zi, q):
        b = block(zi, x, c)
        for j in range(1, n_cen):
            send(b, q, send_c, c_slot(zi, n_cen - j, q), c_peer(j))
        send(b, q, send_x, x_slot(zi, q), x_peer)

    def passes_up(zi):
        return jnp.logical_and(has_up, zi <= z)

    def passes_down(zi):
        return jnp.logical_and(has_down, zi >= z)

    def passes(zi):
        return jnp.logical_or(passes_up(zi), passes_down(zi))

    def line_arrived(zi, q):
        arrived(allc.at[block(zi, x, c), rows_of(q)], line_sem.at[zi, q])

    def straight(i, q):
        zi = ordered(i)
        b = block(zi, x, c)
        for j in range(1, n_cen):
            pl.when(jnp.abs(zi - z) > 1)(
                functools.partial(
                    send, b, q, send_dx if q < HALF else send_dc,
                    d_slot(zi, n_cen - j, q), at(z, 1 - x, c_at(j)),
                )
            )

    def line_forward(d, q):
        def visit(zi):
            @pl.when(passes(zi))
            def _():
                line_arrived(zi, q)
                along(zi, q)

        at_distance(d, visit)

    def line_step(i, q):
        zi = ordered(i)
        pl.when(jnp.logical_not(passes(zi)))(lambda: line_arrived(zi, q))

    def ordered(i):
        near = jnp.minimum(z, n_z - 1 - z)
        beside = z + (i + 1) // 2 if i % 2 else z - i // 2
        beyond = jnp.where(z <= n_z - 1 - z, i, n_z - 1 - i)
        return jnp.where(i <= 2 * near, beside, beyond)

    def d_slot(zi, j, q):
        return d_sem.at[seat(zi, j), q]

    def by_line(q):
        return q in LINE_PIECES

    def cross_step(i, q):
        zi = ordered(i)

        def forward(visit):
            if i == 0:
                visit()
            elif not by_line(q):
                pl.when(jnp.abs(zi - z) > 1)(visit)

        for j in range(1, n_cen):
            if q < HALF:
                b = block(zi, x, c_at(j))
                arrived(allc.at[b, rows_of(q)], c_slot(zi, j, q))
                forward(functools.partial(send, b, q, send_dx, d_slot(zi, j, q), x_peer))
        if q >= HALF:
            b = block(zi, 1 - x, c)
            arrived(allc.at[b, rows_of(q)], x_slot(zi, q))
            for j in range(1, n_cen):
                forward(
                    functools.partial(send, b, q, send_dc, d_slot(zi, n_cen - j, q), c_peer(j))
                )

    def last_of(at_z):
        return jnp.where(at_z <= n_z - 1 - at_z, n_z - 1, 0)

    def onward(zi, q):
        up, down = passes_up(zi), passes_down(zi)
        if q != LINE_PIECES[0] and n_z > 2:
            up = jnp.logical_and(up, zi != last_of(z + 1))
            down = jnp.logical_and(down, zi != last_of(z - 1))
        return up, down

    def diagonal_step(d, q):
        def visit(zi):
            for j in range(1, n_cen):
                b = block(zi, 1 - x, c_at(j))
                slot = d_slot(zi, j, q)
                up, down = onward(zi, q)
                pl.when(jnp.logical_or(up, down))(
                    functools.partial(arrived, allc.at[b, rows_of(q)], slot)
                )
                pl.when(up)(functools.partial(send, b, q, send_dup, slot, up_peer))
                pl.when(down)(functools.partial(send, b, q, send_ddown, slot, down_peer))

        at_distance(d, visit)

    def corner_ready(zi, j):
        b = block(zi, 1 - x, c_at(j))
        for q in range(PIECES):
            seen = jnp.logical_or(*onward(zi, q)) if by_line(q) else zi == z
            pl.when(jnp.logical_not(seen))(
                functools.partial(arrived, allc.at[b, rows_of(q)], d_slot(zi, j, q))
            )

    with jax.named_scope("load"):
        load_states.wait()
        load_first.wait()
        load_bias.wait()
        load_cen.start()
    part = n // 2
    for h in range(2):
        rows = pl.ds(h * part, part)
        with jax.named_scope(f"encode{h}"):
            pre = jnp.dot(states_ref[rows, :], first_ref[...], preferred_element_type=jnp.float32)
            hidden = jax.nn.gelu(pre + bias_ref[...][None, :]).astype(jnp.bfloat16)
            if h == 0:
                load_second.wait()
            allc[mine, rows, :] = jnp.dot(
                hidden, second_ref[...], preferred_element_type=jnp.float32
            ).astype(jnp.bfloat16)
        if h == 0:
            with jax.named_scope("barrier"):
                pl.semaphore_wait(barrier, greetings)
        for q in range(h * HALF, (h + 1) * HALF):
            along(z, ORDER[q])
            aside(z, q)

    def tell(i, peer):
        pl.semaphore_signal(token.at[i], inc=1, device_id=peer, device_id_type=MESH)

    pl.when(z == 0)(lambda: tell(0, up_peer))
    pl.when(z == n_z - 1)(lambda: tell(1, down_peer))

    def pass_on(s):
        @pl.when(jnp.logical_and(has_down, z == s + 1))
        def _():
            pl.semaphore_wait(token.at[0], 1)
            pl.when(has_up)(lambda: tell(0, up_peer))

        @pl.when(jnp.logical_and(has_up, 2 * (n_z - 2 - z) == s))
        def _():
            pl.semaphore_wait(token.at[1], 1)
            pl.when(has_down)(lambda: tell(1, down_peer))

        if s == 2 * (n_z - 2):
            tell(2, x_peer)

    tile = min(512, cen_ref.shape[0])
    tiles = cen_ref.shape[0] // tile
    scale = 2.0 * LOG2E / smoothing_scale

    def tile_rows(i):
        return pl.ds(i * tile, tile) if isinstance(i, int) else pl.ds(pl.multiple_of(i * tile, tile), tile)

    def square_step(i):
        wide = cen_ref[tile_rows(i), :].astype(jnp.float32)
        total = jnp.sum(wide * wide, axis=1, keepdims=True) * (LOG2E / smoothing_scale)
        squares[tile_rows(i), :] = jnp.broadcast_to(total, (tile, 128))

    def less_squares(scores, rows):
        offset = squares[rows, :]
        return jnp.concatenate(
            [scores[:, q * 128:(q + 1) * 128] * scale - offset for q in range(scores.shape[1] // 128)],
            axis=1,
        )

    def stats_step(rows, i, carry):
        peak, total = carry
        scores = lax.dot_general(
            cen_ref[tile_rows(i), :], rows, NT, preferred_element_type=jnp.float32
        )
        scores = less_squares(scores, tile_rows(i)).reshape(tile // 8, 8, rows.shape[0])
        peak_next = jnp.maximum(peak, jnp.max(scores, axis=0))
        total_next = total * jnp.exp2(peak - peak_next) + jnp.sum(
            jnp.exp2(scores - peak_next[None]), axis=0
        )
        return peak_next, total_next

    group_rows = n * n_cen

    def keep_stats(j, carry):
        peak, total = carry
        top = jnp.max(peak, axis=0, keepdims=True)
        mass = jnp.sum(total * jnp.exp2(peak - top), axis=0, keepdims=True)
        start = pl.multiple_of(c_at(j) * n, n)
        stat[c, :, pl.ds(start, top.shape[1])] = top
        stat[c, :, pl.ds(group_rows + start, top.shape[1])] = mass

    def fresh(count):
        return jnp.full((8, count), -jnp.inf, jnp.float32), jnp.zeros((8, count), jnp.float32)

    with jax.named_scope("cen"):
        load_cen.wait()
    with jax.named_scope("stats_own"):
        running = fresh(n)
        for i in range(tiles):
            square_step(i)
            running = stats_step(allc[mine], i, running)
        keep_stats(0, running)
    wide = allc[mine].astype(jnp.float32)
    lengths = lax.dot_general(
        jnp.ones((8, width), jnp.float32), wide * wide, NT,
        preferred_element_type=jnp.float32, precision=lax.Precision.HIGHEST,
    )
    weighted[...] = jnp.zeros_like(weighted)
    counts[...] = jnp.zeros_like(counts)

    both = pl.ds(pl.multiple_of((p - core) * n_own, 2 * n_own), 2 * n_own)

    def consume(b, g, ci, count=1, owner=None):
        span = count * n
        rows = allc[pl.ds(b, count)].reshape(span, width)
        pair, seats = both, slice(None)
        if owner is not None:
            pair = pl.ds(pl.multiple_of((p - core + owner) * n_own, n_own), n_own)
            seats = pl.ds(owner, 1)
        scores = lax.dot_general(cen_ref[pair, :], rows, NT, preferred_element_type=jnp.float32)
        level = norm[g, :, pl.ds(pl.multiple_of(ci * n, n), span)]
        resp = jnp.exp2(less_squares(scores, pair) - level)
        lanes = resp[:, 0:128]
        for q in range(1, span // 128):
            lanes = lanes + resp[:, q * 128:(q + 1) * 128]
        counts[seats] += lanes.reshape(-1, n_own, 128)
        weighted[seats] += jnp.dot(
            resp.astype(jnp.bfloat16), rows, preferred_element_type=jnp.float32
        ).reshape(-1, n_own, width)

    def consume_group(g, owner=None):
        if n_cen <= 2:
            consume(g * n_cen, g, 0, n_cen, owner=owner)
            return

        def one(ci, _):
            consume(g * n_cen + ci, g, ci, owner=owner)
            return 0

        lax.fori_loop(0, n_cen, one, 0)

    def rest_of(b, q, sem):
        arrived(allc.at[b, rows_of(q, HALF)], sem)

    def norm_arrived(zi, xi):
        g = zi * 2 + xi
        arrived(norm.at[g], norm_sem.at[g])

    def line_ready(i):
        zi = ordered(i)
        if i > 0:
            norm_arrived(zi, x)
            for j in range(1, n_cen):
                b = block(zi, x, c_at(j))
                for q in range(HALF):
                    if by_line(q) or i == n_z - 1:
                        arrived(allc.at[b, rows_of(q)], c_slot(zi, j, q))
                rest_of(b, HALF, c_rest.at[seat(zi, j)])

    def x_ready(i):
        zi = ordered(i)
        norm_arrived(zi, 1 - x)
        b = block(zi, 1 - x, c)
        rest_of(b, 0, x_rest.at[zi])
        if i > 0:
            for q in range(HALF, PIECES):
                if by_line(q) or i == n_z - 1:
                    arrived(allc.at[b, rows_of(q)], x_slot(zi, q))

    def cross_ready(i):
        x_ready(i)
        for j in range(1, n_cen):
            corner_ready(ordered(i), j)

    def take_line(i, owner=None):
        consume_group(ordered(i) * 2 + x, owner)

    def take_cross(i, owner=None):
        consume_group(ordered(i) * 2 + 1 - x, owner)

    def take_last_b(i, owner):
        zi = ordered(i)
        consume(block(zi, 1 - x, c), zi * 2 + 1 - x, c, owner=owner)

    def take_last_d(i, owner):
        zi = ordered(i)
        for j in range(1, n_cen):
            consume(block(zi, 1 - x, c_at(j)), zi * 2 + 1 - x, c_at(j), owner=owner)

    def cross_stats(j):
        b = block(z, x, c_at(j))

        def step(i, carry):
            return stats_step(allc[b], i, carry)

        running = fresh(n)
        if n_cen <= 2:
            for i in range(tiles):
                running = step(i, running)
        else:
            running = lax.fori_loop(0, tiles, step, running)
        keep_stats(j, running)

    def share_stats():
        for j in range(1, n_cen):
            remote(
                stat.at[c], stat.at[c], send_stat, stat_sem.at[n_cen - j - 1], c_peer(j)
            ).start()

    def share_norm():
        for j in range(1, n_cen):
            s = c_at(j)
            arrived(stat.at[s], stat_sem.at[j - 1])
        top = stat[0, :, 0:group_rows]
        for s in range(1, n_cen):
            top = jnp.maximum(top, stat[s, :, 0:group_rows])
        mass = jnp.zeros_like(top)
        for s in range(n_cen):
            mass = mass + stat[s, :, group_rows:2 * group_rows] * jnp.exp2(
                stat[s, :, 0:group_rows] - top
            )
        level = top + jnp.log(mass) * LOG2E
        g = z * 2 + x
        norm[g] = level
        pl.semaphore_wait(token.at[2], 1)
        for k in range(1, 2 * n_z):
            h = lax.rem(g + k, 2 * n_z)
            remote(norm.at[g], norm.at[g], send_norm, norm_sem.at[g], at(h // 2, lax.rem(h, 2), c)).start()
        own = norm[g, :, pl.ds(pl.multiple_of(c * n, n), n)]
        pen_ref[...] = (-(smoothing_scale / width)) * (
            own * math.log(2.0) - lengths[0:1, :] / smoothing_scale
        )

    total_steps = n_z * PIECES
    norm_at = 2 * PIECES - 1

    diagonals = {}
    for q, s in enumerate((1, 3, 2, 3)):
        diagonals.setdefault(min(PIECES + s, total_steps - 1), []).append((0, q))
    for d in range(1, n_z):
        for e in range(2):
            s = min(2 * PIECES + 1 + 3 * (d - 1) + e, total_steps - 1)
            diagonals.setdefault(s, []).append((d, LINE_PIECES[e]))
    for s in range(total_steps):
        i, q = 1 + s // PIECES, s % PIECES
        with jax.named_scope(f"move{s}"):
            if i < n_z:
                if i == 1:
                    line_forward(1, ORDER[q])
                line_step(i, ORDER[q])
                if i == 1:
                    cross_step(0, q)
                if i == n_z - 1 and ORDER[q] != LINE_PIECES[0]:
                    straight(i, ORDER[q])
                aside(ordered(i), ORDER[q])
                if i > 1 and q < 2:
                    for ahead in ORDER[:-1] if q == 0 else ORDER[-1:]:
                        line_forward(i, ahead)
            if 1 < i < n_z and q % 2 == 0:
                cross_step(i - 1, q + 1)
            for d, piece_index in diagonals.get(s, ()):
                diagonal_step(d, piece_index)
            if s <= max(n_z - 2, 2 * (n_z - 2)):
                pass_on(s)
        with jax.named_scope(f"work{s}"):
            if s == PIECES - 1:
                for j in range(1, n_cen):
                    rest_of(block(z, x, c_at(j)), HALF, c_rest.at[seat(z, j)])
                    cross_stats(j)
                share_stats()
            if s == norm_at:
                share_norm()
                take_line(0)
    last = n_z - 1
    takes = []
    for i in range(1, n_z):
        takes += [
            (functools.partial(line_ready, i), functools.partial(take_line, i)),
            (functools.partial(cross_ready, i - 1), functools.partial(take_cross, i - 1)),
        ]
    takes.append((functools.partial(x_ready, last), functools.partial(take_last_b, last)))
    split = len(takes) - 3
    with jax.named_scope("tail"):
        for k, (ready, take) in enumerate(takes):
            ready()
            take(owner=None if k < split else 1 - core)

    with jax.named_scope("sent"):

        def left(ref, send_sem):
            remote(ref, ref, send_sem, line_sem.at[z, 0], core_peer).wait_send()

        left(allc.at[pl.ds(0, n_z)], send_x)
        left(allc.at[pl.ds(0, others * n_z)], send_c)

        def left_corner(near):
            corner = others * (HALF + (n_z - 1 - near) * (HALF - 1))
            extra = others if n_z > 2 else 0
            left(allc.at[pl.ds(0, corner), rows_of(0)], send_dx)
            left(allc.at[pl.ds(0, corner + extra), rows_of(0)], send_dc)

        inside = jnp.logical_and(has_up, has_down)
        pl.when(inside)(lambda: left_corner(2))
        pl.when(jnp.logical_not(inside))(lambda: left_corner(1))

        def left_line(count, whole, parts):
            left(allc.at[pl.ds(0, count)], whole)
            pieces = others * (2 * (count + 1) - (1 if 2 * count >= n_z > 2 else 0))
            left(allc.at[pl.ds(0, pieces), rows_of(0)], parts)

        for zi in range(n_z - 1):
            pl.when(z == zi)(functools.partial(left_line, zi + 1, send_up, send_dup))
            pl.when(z == n_z - 1 - zi)(
                functools.partial(left_line, zi + 1, send_down, send_ddown)
            )
        left(stat.at[pl.ds(0, others)], send_stat)
        left(norm.at[pl.ds(0, 2 * n_z - 1)], send_norm)

    with jax.named_scope("tail_d"):
        for j in range(1, n_cen):
            corner_ready(ordered(last), j)
        take_last_d(last, 1 - core)

    with jax.named_scope("pair"):
        sums = remote(
            weighted.at[1 - core], other_sums, send_x, line_sem.at[z, 0], core_peer
        )
        tally = remote(
            counts.at[1 - core], other_counts, send_c, line_sem.at[z, 1], core_peer
        )
        tally.start()
        sums.start()
        for _, take in takes[split:]:
            take(owner=core)
        take_last_d(last, core)
        own_rows = pl.ds(pl.multiple_of(p * n_own, n_own), n_own)
        tally.wait()
        share = 1.0 / (
            jnp.sum(counts[core] + other_counts[...], axis=1, keepdims=True) + 1.0
        )
        sums.wait()
    with jax.named_scope("final"):
        out_ref[...] = (
            weighted[core] + other_sums[...] + cen_ref[own_rows, :].astype(jnp.float32)
        ) * share


def finish(fresh_ref, pen_ref, out_ref, cost_ref):
    out_ref[0] = fresh_ref[...]
    cost_ref[...] = pen_ref[0]


def body(n_pts, n_cen, states, first_weight, first_bias, second_weight, centroids):
    n, width = states.shape[0], second_weight.shape[1]
    k_dev = centroids.shape[1]
    owned = k_dev // n_pts
    n_z, others = n_pts // 4, n_cen - 1
    dma = pltpu.SemaphoreType.DMA
    vmem, f32 = pltpu.VMEM, jnp.float32
    args = [
        pltpu.with_memory_space_constraint(v, pltpu.HBM)
        for v in (states, first_weight, first_bias, second_weight, centroids)
    ]
    fresh, penalty = pl.pallas_call(
        functools.partial(kernel, n_pts, n_cen),
        out_shape=(vmem((owned, width), f32), vmem((1, n), f32)),
        in_specs=[pl.BlockSpec(memory_space=pltpu.HBM)] * 5,
        out_specs=(pl.BlockSpec(memory_space=vmem),) * 2,
        scratch_shapes=[
            vmem(states.shape, states.dtype),
            vmem(first_weight.shape, first_weight.dtype),
            vmem(first_bias.shape, first_bias.dtype),
            vmem(second_weight.shape, second_weight.dtype),
            vmem(centroids.shape[1:], centroids.dtype),
            vmem((2 * n_z * n_cen, n, width), jnp.bfloat16),
            vmem((n_cen, 1, 2 * n_cen * n), f32),
            vmem((2 * n_z, 1, n_cen * n), f32),
            vmem((k_dev, 128), f32),
            vmem((2, owned, width), f32),
            vmem((2, owned, 128), f32),
            vmem((owned, width), f32),
            vmem((owned, 128), f32),
            dma((n_z, PIECES)),
            dma((n_z * others, HALF)),
            dma((n_z * others,)),
            dma((n_z, HALF)),
            dma((n_z,)),
            dma((n_z * others, PIECES)),
            dma((others,)),
            dma((2 * n_z,)),
            *([dma] * 10),
            pltpu.SemaphoreType.REGULAR((3,)),
        ],
        compiler_params=pltpu.CompilerParams(
            collective_id=0, has_side_effects=True, vmem_limit_bytes=48 * 1024 * 1024
        ),
    )(*args)
    return pl.pallas_call(
        finish,
        out_shape=(
            jax.ShapeDtypeStruct((1, owned, width), f32),
            jax.ShapeDtypeStruct((n,), f32),
        ),
        in_specs=[pl.BlockSpec(memory_space=vmem)] * 2,
        out_specs=(pl.BlockSpec(memory_space=vmem),) * 2,
        compiler_params=pltpu.CompilerParams(vmem_limit_bytes=4 * 1024 * 1024),
    )(fresh, penalty)


def solution(mesh):
    placed = (P(("pts", "cen"), None), P(), P(), P(), P("cen", None, None))
    return jax.shard_map(
        functools.partial(body, mesh.shape["pts"], mesh.shape["cen"]),
        mesh=mesh,
        in_specs=placed,
        out_specs=(P("cen", "pts", None), P(("pts", "cen"))),
        check_vma=False,
    )
```

```python
import functools
import math

import jax
import jax.numpy as jnp
from jax import lax
from jax.experimental import pallas as pl
from jax.experimental.pallas import tpu as pltpu
from jax.sharding import PartitionSpec as P

smoothing_scale = 16.0
LOG2E = math.log2(math.e)
MESH = pl.DeviceIdType.MESH
NT = (((1,), (1,)), ((), ()))
PIECES = 4
HALF = PIECES // 2
LINE_PIECES = (0, HALF)
ORDER = (1, 0, 3, 2)


def kernel(
    n_pts, n_cen, states_hbm, first_hbm, bias_hbm, second_hbm, cen_hbm, out_ref, pen_ref,
    states_ref, first_ref, bias_ref, second_ref, cen_ref,
    allc, stat, norm, squares, weighted, counts, other_sums, other_counts,
    line_sem, c_sem, c_rest, x_sem, x_rest, d_sem, stat_sem, norm_sem,
    send_up, send_down, send_x, send_c, send_dup, send_ddown, send_dx, send_dc,
    send_stat, send_norm, token,
):
    n, width = states_ref.shape[0], second_ref.shape[1]
    n_z, others = n_pts // 4, n_cen - 1
    n_own = out_ref.shape[0]
    piece = n // PIECES

    def load(i, src, dst):
        return pltpu.make_async_copy(src, dst, (send_x, send_c, send_dx, send_dc, send_stat)[i])

    load_states = load(0, states_hbm, states_ref)
    load_first = load(1, first_hbm, first_ref)
    load_bias = load(2, bias_hbm, bias_ref)
    load_second = load(3, second_hbm, second_ref)
    load_cen = load(4, cen_hbm.at[0], cen_ref)
    def start(i, src, dst, parts):
        rows = dst.shape[0] // parts
        for k in range(parts):
            at_rows = pl.ds(k * rows, rows)
            load(i, src.at[at_rows], dst.at[at_rows]).start()

    start(0, states_hbm, states_ref, 1)
    start(1, first_hbm, first_ref, 4)
    load_bias.start()
    start(3, second_hbm, second_ref, 2)

    p, c = lax.axis_index("pts"), lax.axis_index("cen")
    core, x, z = lax.rem(p, 2), lax.rem(p // 2, 2), p // 4
    has_up, has_down = z < n_z - 1, z > 0

    side = lax.rem(core + x + z + c, 2)

    def at(zi, xi, ci):
        return ((zi * 2 + xi) * 2 + lax.rem(side + xi + zi + ci, 2), ci)

    def c_at(j):
        return lax.rem(c + j, n_cen)

    def block(zi, xi, ci):
        return (zi * 2 + xi) * n_cen + ci

    def c_peer(j):
        return at(z, x, c_at(j))

    up_peer, down_peer = at(lax.rem(z + 1, n_z), x, c), at(lax.rem(z + n_z - 1, n_z), x, c)
    x_peer, core_peer = at(z, 1 - x, c), (p + 1 - 2 * core, c)
    mine = block(z, x, c)

    barrier = pltpu.get_barrier_semaphore()

    def greet(peer):
        pl.semaphore_signal(barrier, inc=1, device_id=peer, device_id_type=MESH)

    pl.when(has_up)(lambda: greet(up_peer))
    pl.when(has_down)(lambda: greet(down_peer))
    greet(x_peer)
    greet(core_peer)
    for j in range(1, n_cen):
        greet(c_peer(j))
    greetings = 2 + others + has_up.astype(jnp.int32) + has_down.astype(jnp.int32)

    def rows_of(q, count=1):
        return pl.ds(q * piece, count * piece)

    def remote(src, dst, send, recv, peer):
        return pltpu.make_async_remote_copy(
            src_ref=src, dst_ref=dst, send_sem=send, recv_sem=recv,
            device_id=peer, device_id_type=MESH,
        )

    def send(b, q, send_sem, recv_sem, peer):
        ref = allc.at[b, rows_of(q)]
        remote(ref, ref, send_sem, recv_sem, peer).start()

    def arrived(ref, recv_sem):
        remote(ref, ref, send_x, recv_sem, core_peer).wait_recv()

    def seat(zi, j):
        return zi * others + j - 1

    def c_slot(zi, j, q):
        return c_sem.at[seat(zi, j), q] if q < HALF else c_rest.at[seat(zi, j)]

    def x_slot(zi, q):
        return x_rest.at[zi] if q < HALF else x_sem.at[zi, q - HALF]

    def at_distance(d, visit):
        if d == 0:
            visit(z)
            return
        pl.when(z + d < n_z)(lambda: visit(z + d))
        pl.when(z >= d)(lambda: visit(z - d))

    def along(zi, q):
        b = block(zi, x, c)
        pl.when(passes_up(zi))(lambda: send(b, q, send_up, line_sem.at[zi, q], up_peer))
        pl.when(passes_down(zi))(lambda: send(b, q, send_down, line_sem.at[zi, q], down_peer))

    def aside(zi, q):
        b = block(zi, x, c)
        for j in range(1, n_cen):
            send(b, q, send_c, c_slot(zi, n_cen - j, q), c_peer(j))
        send(b, q, send_x, x_slot(zi, q), x_peer)

    def passes_up(zi):
        return jnp.logical_and(has_up, zi <= z)

    def passes_down(zi):
        return jnp.logical_and(has_down, zi >= z)

    def passes(zi):
        return jnp.logical_or(passes_up(zi), passes_down(zi))

    def line_arrived(zi, q):
        arrived(allc.at[block(zi, x, c), rows_of(q)], line_sem.at[zi, q])

    def straight(i, q):
        zi = ordered(i)
        b = block(zi, x, c)
        for j in range(1, n_cen):
            pl.when(jnp.abs(zi - z) > 1)(
                functools.partial(
                    send, b, q, send_dx if q < HALF else send_dc,
                    d_slot(zi, n_cen - j, q), at(z, 1 - x, c_at(j)),
                )
            )

    def line_forward(d, q):
        def visit(zi):
            @pl.when(passes(zi))
            def _():
                line_arrived(zi, q)
                along(zi, q)

        at_distance(d, visit)

    def line_step(i, q):
        zi = ordered(i)
        pl.when(jnp.logical_not(passes(zi)))(lambda: line_arrived(zi, q))

    def ordered(i):
        near = jnp.minimum(z, n_z - 1 - z)
        beside = z + (i + 1) // 2 if i % 2 else z - i // 2
        beyond = jnp.where(z <= n_z - 1 - z, i, n_z - 1 - i)
        return jnp.where(i <= 2 * near, beside, beyond)

    def d_slot(zi, j, q):
        return d_sem.at[seat(zi, j), q]

    def by_line(q):
        return q in LINE_PIECES

    def cross_step(i, q):
        zi = ordered(i)

        def forward(visit):
            if i == 0:
                visit()
            elif not by_line(q):
                pl.when(jnp.abs(zi - z) > 1)(visit)

        for j in range(1, n_cen):
            if q < HALF:
                b = block(zi, x, c_at(j))
                arrived(allc.at[b, rows_of(q)], c_slot(zi, j, q))
                forward(functools.partial(send, b, q, send_dx, d_slot(zi, j, q), x_peer))
        if q >= HALF:
            b = block(zi, 1 - x, c)
            arrived(allc.at[b, rows_of(q)], x_slot(zi, q))
            for j in range(1, n_cen):
                forward(
                    functools.partial(send, b, q, send_dc, d_slot(zi, n_cen - j, q), c_peer(j))
                )

    def last_of(at_z):
        return jnp.where(at_z <= n_z - 1 - at_z, n_z - 1, 0)

    def onward(zi, q):
        up, down = passes_up(zi), passes_down(zi)
        if q != LINE_PIECES[0] and n_z > 2:
            up = jnp.logical_and(up, zi != last_of(z + 1))
            down = jnp.logical_and(down, zi != last_of(z - 1))
        return up, down

    def diagonal_step(d, q):
        def visit(zi):
            for j in range(1, n_cen):
                b = block(zi, 1 - x, c_at(j))
                slot = d_slot(zi, j, q)
                up, down = onward(zi, q)
                pl.when(jnp.logical_or(up, down))(
                    functools.partial(arrived, allc.at[b, rows_of(q)], slot)
                )
                pl.when(up)(functools.partial(send, b, q, send_dup, slot, up_peer))
                pl.when(down)(functools.partial(send, b, q, send_ddown, slot, down_peer))

        at_distance(d, visit)

    def corner_ready(zi, j):
        b = block(zi, 1 - x, c_at(j))
        for q in range(PIECES):
            seen = jnp.logical_or(*onward(zi, q)) if by_line(q) else zi == z
            pl.when(jnp.logical_not(seen))(
                functools.partial(arrived, allc.at[b, rows_of(q)], d_slot(zi, j, q))
            )

    with jax.named_scope("load"):
        load_states.wait()
        load_first.wait()
        load_bias.wait()
        load_cen.start()
    part = n // 2
    for h in range(2):
        rows = pl.ds(h * part, part)
        with jax.named_scope(f"encode{h}"):
            pre = jnp.dot(states_ref[rows, :], first_ref[...], preferred_element_type=jnp.float32)
            hidden = jax.nn.gelu(pre + bias_ref[...][None, :]).astype(jnp.bfloat16)
            if h == 0:
                load_second.wait()
            allc[mine, rows, :] = jnp.dot(
                hidden, second_ref[...], preferred_element_type=jnp.float32
            ).astype(jnp.bfloat16)
        if h == 0:
            with jax.named_scope("barrier"):
                pl.semaphore_wait(barrier, greetings)
        for q in range(h * HALF, (h + 1) * HALF):
            along(z, ORDER[q])
            aside(z, q)

    def tell(i, peer):
        pl.semaphore_signal(token.at[i], inc=1, device_id=peer, device_id_type=MESH)

    pl.when(z == 0)(lambda: tell(0, up_peer))
    pl.when(z == n_z - 1)(lambda: tell(1, down_peer))

    def pass_on(s):
        @pl.when(jnp.logical_and(has_down, z == s + 1))
        def _():
            pl.semaphore_wait(token.at[0], 1)
            pl.when(has_up)(lambda: tell(0, up_peer))

        @pl.when(jnp.logical_and(has_up, 2 * (n_z - 2 - z) == s))
        def _():
            pl.semaphore_wait(token.at[1], 1)
            pl.when(has_down)(lambda: tell(1, down_peer))

        if s == 2 * (n_z - 2):
            tell(2, x_peer)

    tile = min(512, cen_ref.shape[0])
    tiles = cen_ref.shape[0] // tile
    scale = 2.0 * LOG2E / smoothing_scale

    def tile_rows(i):
        return pl.ds(i * tile, tile) if isinstance(i, int) else pl.ds(pl.multiple_of(i * tile, tile), tile)

    def square_step(i):
        wide = cen_ref[tile_rows(i), :].astype(jnp.float32)
        total = jnp.sum(wide * wide, axis=1, keepdims=True) * (LOG2E / smoothing_scale)
        squares[tile_rows(i), :] = jnp.broadcast_to(total, (tile, 128))

    def less_squares(scores, rows):
        offset = squares[rows, :]
        return jnp.concatenate(
            [scores[:, q * 128:(q + 1) * 128] * scale - offset for q in range(scores.shape[1] // 128)],
            axis=1,
        )

    def stats_step(rows, i, carry):
        peak, total = carry
        scores = lax.dot_general(
            cen_ref[tile_rows(i), :], rows, NT, preferred_element_type=jnp.float32
        )
        scores = less_squares(scores, tile_rows(i)).reshape(tile // 8, 8, rows.shape[0])
        peak_next = jnp.maximum(peak, jnp.max(scores, axis=0))
        total_next = total * jnp.exp2(peak - peak_next) + jnp.sum(
            jnp.exp2(scores - peak_next[None]), axis=0
        )
        return peak_next, total_next

    group_rows = n * n_cen

    def keep_stats(j, carry):
        peak, total = carry
        top = jnp.max(peak, axis=0, keepdims=True)
        mass = jnp.sum(total * jnp.exp2(peak - top), axis=0, keepdims=True)
        start = pl.multiple_of(c_at(j) * n, n)
        stat[c, :, pl.ds(start, top.shape[1])] = top
        stat[c, :, pl.ds(group_rows + start, top.shape[1])] = mass

    def fresh(count):
        return jnp.full((8, count), -jnp.inf, jnp.float32), jnp.zeros((8, count), jnp.float32)

    with jax.named_scope("cen"):
        load_cen.wait()
    with jax.named_scope("stats_own"):
        running = fresh(n)
        for i in range(tiles):
            square_step(i)
            running = stats_step(allc[mine], i, running)
        keep_stats(0, running)
    wide = allc[mine].astype(jnp.float32)
    lengths = lax.dot_general(
        jnp.ones((8, width), jnp.float32), wide * wide, NT,
        preferred_element_type=jnp.float32, precision=lax.Precision.HIGHEST,
    )
    weighted[...] = jnp.zeros_like(weighted)
    counts[...] = jnp.zeros_like(counts)

    both = pl.ds(pl.multiple_of((p - core) * n_own, 2 * n_own), 2 * n_own)

    def consume(b, g, ci, count=1, owner=None):
        span = count * n
        rows = allc[pl.ds(b, count)].reshape(span, width)
        pair, seats = both, slice(None)
        if owner is not None:
            pair = pl.ds(pl.multiple_of((p - core + owner) * n_own, n_own), n_own)
            seats = pl.ds(owner, 1)
        scores = lax.dot_general(cen_ref[pair, :], rows, NT, preferred_element_type=jnp.float32)
        level = norm[g, :, pl.ds(pl.multiple_of(ci * n, n), span)]
        resp = jnp.exp2(less_squares(scores, pair) - level)
        lanes = resp[:, 0:128]
        for q in range(1, span // 128):
            lanes = lanes + resp[:, q * 128:(q + 1) * 128]
        counts[seats] += lanes.reshape(-1, n_own, 128)
        weighted[seats] += jnp.dot(
            resp.astype(jnp.bfloat16), rows, preferred_element_type=jnp.float32
        ).reshape(-1, n_own, width)

    def consume_group(g, owner=None):
        if n_cen <= 2:
            consume(g * n_cen, g, 0, n_cen, owner=owner)
            return

        def one(ci, _):
            consume(g * n_cen + ci, g, ci, owner=owner)
            return 0

        lax.fori_loop(0, n_cen, one, 0)

    def rest_of(b, q, sem):
        arrived(allc.at[b, rows_of(q, HALF)], sem)

    def norm_arrived(zi, xi):
        g = zi * 2 + xi
        arrived(norm.at[g], norm_sem.at[g])

    def line_ready(i):
        zi = ordered(i)
        if i > 0:
            norm_arrived(zi, x)
            for j in range(1, n_cen):
                b = block(zi, x, c_at(j))
                for q in range(HALF):
                    if by_line(q) or i == n_z - 1:
                        arrived(allc.at[b, rows_of(q)], c_slot(zi, j, q))
                rest_of(b, HALF, c_rest.at[seat(zi, j)])

    def x_ready(i):
        zi = ordered(i)
        norm_arrived(zi, 1 - x)
        b = block(zi, 1 - x, c)
        rest_of(b, 0, x_rest.at[zi])
        if i > 0:
            for q in range(HALF, PIECES):
                if by_line(q) or i == n_z - 1:
                    arrived(allc.at[b, rows_of(q)], x_slot(zi, q))

    def cross_ready(i):
        x_ready(i)
        for j in range(1, n_cen):
            corner_ready(ordered(i), j)

    def take_line(i, owner=None):
        consume_group(ordered(i) * 2 + x, owner)

    def take_cross(i, owner=None):
        consume_group(ordered(i) * 2 + 1 - x, owner)

    def take_last_b(i, owner):
        zi = ordered(i)
        consume(block(zi, 1 - x, c), zi * 2 + 1 - x, c, owner=owner)

    def take_last_d(i, owner):
        zi = ordered(i)
        for j in range(1, n_cen):
            consume(block(zi, 1 - x, c_at(j)), zi * 2 + 1 - x, c_at(j), owner=owner)

    def cross_stats(j):
        b = block(z, x, c_at(j))

        def step(i, carry):
            return stats_step(allc[b], i, carry)

        running = fresh(n)
        if n_cen <= 2:
            for i in range(tiles):
                running = step(i, running)
        else:
            running = lax.fori_loop(0, tiles, step, running)
        keep_stats(j, running)

    def share_stats():
        for j in range(1, n_cen):
            remote(
                stat.at[c], stat.at[c], send_stat, stat_sem.at[n_cen - j - 1], c_peer(j)
            ).start()

    def share_norm():
        for j in range(1, n_cen):
            s = c_at(j)
            arrived(stat.at[s], stat_sem.at[j - 1])
        top = stat[0, :, 0:group_rows]
        for s in range(1, n_cen):
            top = jnp.maximum(top, stat[s, :, 0:group_rows])
        mass = jnp.zeros_like(top)
        for s in range(n_cen):
            mass = mass + stat[s, :, group_rows:2 * group_rows] * jnp.exp2(
                stat[s, :, 0:group_rows] - top
            )
        level = top + jnp.log(mass) * LOG2E
        g = z * 2 + x
        norm[g] = level
        pl.semaphore_wait(token.at[2], 1)
        for k in range(1, 2 * n_z):
            h = lax.rem(g + k, 2 * n_z)
            remote(norm.at[g], norm.at[g], send_norm, norm_sem.at[g], at(h // 2, lax.rem(h, 2), c)).start()
        own = norm[g, :, pl.ds(pl.multiple_of(c * n, n), n)]
        pen_ref[...] = (-(smoothing_scale / width)) * (
            own * math.log(2.0) - lengths[0:1, :] / smoothing_scale
        )

    total_steps = n_z * PIECES
    norm_at = 2 * PIECES - 1

    diagonals = {}
    for q, s in enumerate((1, 3, 2, 3)):
        diagonals.setdefault(min(PIECES + s, total_steps - 1), []).append((0, q))
    for d in range(1, n_z):
        for e in range(2):
            s = min(2 * PIECES + 2 + 2 * (d - 1) + e, total_steps - 1)
            diagonals.setdefault(s, []).append((d, LINE_PIECES[e]))
    for s in range(total_steps):
        i, q = 1 + s // PIECES, s % PIECES
        with jax.named_scope(f"move{s}"):
            if i < n_z:
                if i == 1:
                    line_forward(1, ORDER[q])
                line_step(i, ORDER[q])
                if i == 1:
                    cross_step(0, q)
                if i == n_z - 1 and ORDER[q] != LINE_PIECES[0]:
                    straight(i, ORDER[q])
                aside(ordered(i), ORDER[q])
                if i > 1 and q < 2:
                    for ahead in ORDER[:-1] if q == 0 else ORDER[-1:]:
                        line_forward(i, ahead)
            if 1 < i < n_z and q % 2 == 0:
                cross_step(i - 1, q + 1)
            for d, piece_index in diagonals.get(s, ()):
                diagonal_step(d, piece_index)
            if s <= max(n_z - 2, 2 * (n_z - 2)):
                pass_on(s)
        with jax.named_scope(f"work{s}"):
            if s == PIECES - 1:
                for j in range(1, n_cen):
                    rest_of(block(z, x, c_at(j)), HALF, c_rest.at[seat(z, j)])
                    cross_stats(j)
                share_stats()
            if s == norm_at:
                share_norm()
                take_line(0)
    last = n_z - 1
    takes = []
    for i in range(1, n_z):
        takes += [
            (functools.partial(line_ready, i), functools.partial(take_line, i)),
            (functools.partial(cross_ready, i - 1), functools.partial(take_cross, i - 1)),
        ]
    takes.append((functools.partial(x_ready, last), functools.partial(take_last_b, last)))
    split = len(takes) - 3
    with jax.named_scope("tail"):
        for k, (ready, take) in enumerate(takes):
            ready()
            take(owner=None if k < split else 1 - core)

    with jax.named_scope("sent"):

        def left(ref, send_sem):
            remote(ref, ref, send_sem, line_sem.at[z, 0], core_peer).wait_send()

        left(allc.at[pl.ds(0, n_z)], send_x)
        left(allc.at[pl.ds(0, others * n_z)], send_c)

        def left_corner(near):
            corner = others * (HALF + (n_z - 1 - near) * (HALF - 1))
            extra = others if n_z > 2 else 0
            left(allc.at[pl.ds(0, corner), rows_of(0)], send_dx)
            left(allc.at[pl.ds(0, corner + extra), rows_of(0)], send_dc)

        inside = jnp.logical_and(has_up, has_down)
        pl.when(inside)(lambda: left_corner(2))
        pl.when(jnp.logical_not(inside))(lambda: left_corner(1))

        def left_line(count, whole, parts):
            left(allc.at[pl.ds(0, count)], whole)
            pieces = others * (2 * (count + 1) - (1 if 2 * count >= n_z > 2 else 0))
            left(allc.at[pl.ds(0, pieces), rows_of(0)], parts)

        for zi in range(n_z - 1):
            pl.when(z == zi)(functools.partial(left_line, zi + 1, send_up, send_dup))
            pl.when(z == n_z - 1 - zi)(
                functools.partial(left_line, zi + 1, send_down, send_ddown)
            )
        left(stat.at[pl.ds(0, others)], send_stat)
        left(norm.at[pl.ds(0, 2 * n_z - 1)], send_norm)

    with jax.named_scope("tail_d"):
        for j in range(1, n_cen):
            corner_ready(ordered(last), j)
        take_last_d(last, 1 - core)

    with jax.named_scope("pair"):
        sums = remote(
            weighted.at[1 - core], other_sums, send_x, line_sem.at[z, 0], core_peer
        )
        tally = remote(
            counts.at[1 - core], other_counts, send_c, line_sem.at[z, 1], core_peer
        )
        tally.start()
        sums.start()
        for _, take in takes[split:]:
            take(owner=core)
        take_last_d(last, core)
        own_rows = pl.ds(pl.multiple_of(p * n_own, n_own), n_own)
        tally.wait()
        share = 1.0 / (
            jnp.sum(counts[core] + other_counts[...], axis=1, keepdims=True) + 1.0
        )
        sums.wait()
    with jax.named_scope("final"):
        out_ref[...] = (
            weighted[core] + other_sums[...] + cen_ref[own_rows, :].astype(jnp.float32)
        ) * share


def finish(fresh_ref, pen_ref, out_ref, cost_ref):
    out_ref[0] = fresh_ref[...]
    cost_ref[...] = pen_ref[0]


def body(n_pts, n_cen, states, first_weight, first_bias, second_weight, centroids):
    n, width = states.shape[0], second_weight.shape[1]
    k_dev = centroids.shape[1]
    owned = k_dev // n_pts
    n_z, others = n_pts // 4, n_cen - 1
    dma = pltpu.SemaphoreType.DMA
    vmem, f32 = pltpu.VMEM, jnp.float32
    args = [
        pltpu.with_memory_space_constraint(v, pltpu.HBM)
        for v in (states, first_weight, first_bias, second_weight, centroids)
    ]
    fresh, penalty = pl.pallas_call(
        functools.partial(kernel, n_pts, n_cen),
        out_shape=(vmem((owned, width), f32), vmem((1, n), f32)),
        in_specs=[pl.BlockSpec(memory_space=pltpu.HBM)] * 5,
        out_specs=(pl.BlockSpec(memory_space=vmem),) * 2,
        scratch_shapes=[
            vmem(states.shape, states.dtype),
            vmem(first_weight.shape, first_weight.dtype),
            vmem(first_bias.shape, first_bias.dtype),
            vmem(second_weight.shape, second_weight.dtype),
            vmem(centroids.shape[1:], centroids.dtype),
            vmem((2 * n_z * n_cen, n, width), jnp.bfloat16),
            vmem((n_cen, 1, 2 * n_cen * n), f32),
            vmem((2 * n_z, 1, n_cen * n), f32),
            vmem((k_dev, 128), f32),
            vmem((2, owned, width), f32),
            vmem((2, owned, 128), f32),
            vmem((owned, width), f32),
            vmem((owned, 128), f32),
            dma((n_z, PIECES)),
            dma((n_z * others, HALF)),
            dma((n_z * others,)),
            dma((n_z, HALF)),
            dma((n_z,)),
            dma((n_z * others, PIECES)),
            dma((others,)),
            dma((2 * n_z,)),
            *([dma] * 10),
            pltpu.SemaphoreType.REGULAR((3,)),
        ],
        compiler_params=pltpu.CompilerParams(
            collective_id=0, has_side_effects=True, vmem_limit_bytes=48 * 1024 * 1024
        ),
    )(*args)
    return pl.pallas_call(
        finish,
        out_shape=(
            jax.ShapeDtypeStruct((1, owned, width), f32),
            jax.ShapeDtypeStruct((n,), f32),
        ),
        in_specs=[pl.BlockSpec(memory_space=vmem)] * 2,
        out_specs=(pl.BlockSpec(memory_space=vmem),) * 2,
        compiler_params=pltpu.CompilerParams(vmem_limit_bytes=4 * 1024 * 1024),
    )(fresh, penalty)


def solution(mesh):
    placed = (P(("pts", "cen"), None), P(), P(), P(), P("cen", None, None))
    return jax.shard_map(
        functools.partial(body, mesh.shape["pts"], mesh.shape["cen"]),
        mesh=mesh,
        in_specs=placed,
        out_specs=(P("cen", "pts", None), P(("pts", "cen"))),
        check_vma=False,
    )
```
